256 devices in a mesh: expert: 64 (over x, z, core), tensor: 4 (over y).
Axes of the slice: x: 4, y: 4, z: 8, core: 2. Of those that a mesh axis runs over, the one named last changes fastest.
Arguments:
- tokens: bfloat16 [8192, 3584], P('expert', 'tensor'), may hold values from -6 to 6
- expert_ids: int32 [8192, 4], P('expert'), may hold values from 0 to 63, all different within a row; in each aligned block of 128 rows (0 to 127, 128 to 255, ...) at most 12 rows name the same one
- gate_values: bfloat16 [8192, 4], P('expert'), may hold values from 0.049804688 to 0.3984375
- w_gate: bfloat16 [64, 3584, 1024], P('expert', None, 'tensor'), may hold values from -0.09375 to 0.09375
- w_up: bfloat16 [64, 3584, 1024], P('expert', None, 'tensor'), may hold values from -0.09375 to 0.09375
- w_down: bfloat16 [64, 1024, 3584], P('expert', 'tensor'), may hold values from -0.1875 to 0.1875
- shared_gate: bfloat16 [3584, 1024], P(None, 'tensor'), may hold values from -0.09375 to 0.09375
- shared_up: bfloat16 [3584, 1024], P(None, 'tensor'), may hold values from -0.09375 to 0.09375
- shared_down: bfloat16 [1024, 3584], P('tensor'), may hold values from -0.1875 to 0.1875
Outputs:
- moe_output: bfloat16 [8192, 3584], P('expert', 'tensor')
The draws below stay inside these ranges and needn't reach their ends.
Inputs may be any that keep to these rules, and one draw needn't show every extreme that they name: `expert_ids`: each token names 4 different experts. Among the 128 tokens of one index of the expert axis (aligned blocks of 128 rows) no expert is named by more than 12 tokens, a bound that some block reaches.
All inputs are finite; a program needn't handle non-finite values.
Results may differ from the reference program's by a relative error of at most 0.013.
Values may be sent and summed in bfloat16 or wider, within the bound.
No kernel may reach another device: no remote copies, remote signals or barrier semaphores. Data moves between devices by JAX's collectives and lax.ppermute only.
A program may use at most 64 MiB of HBM per device.

```python
import math
import jax
import jax.numpy as jnp
import numpy as np
from jax import lax

D = 3584
FF = 1024
SFF = 1024
TOPK = 4
TOK_DEV = 128
EXPERTS = 64
CAP = 12
TOKENS = 8192
N_TENSOR = 4


def block_scale(key, shape, pieces, smallest, largest):
    level = 1.0
    for axis_at, shards_of in pieces:
        steps = jax.random.uniform(jax.random.fold_in(jax.random.fold_in(key, 6), axis_at), (shards_of,), jnp.float32, smallest / len(pieces), largest / len(pieces))
        level = level * jnp.repeat(jnp.exp(steps), shape[axis_at] // shards_of).reshape((-1,) + (1,) * (len(shape) - 1 - axis_at))
    return level


def assign_block(rng, own, number, rows, number_of, top, limit, lean):
    order = jax.random.permutation(rng, number_of)
    crowded, usual = load_shares(number_of, rows * top, limit, lean, True), load_shares(number_of, rows * top, limit, lean, False)
    places = jnp.arange(number_of)

    def named(lengths, turn):
        used = int((lengths > 0).sum())
        fixed = max(1, used // 4)
        passed = fixed + (places - fixed + turn * (used - fixed)) % max(1, number_of - fixed)
        return jnp.zeros((number_of,), jnp.int32).at[order[jnp.where(places < fixed, places, passed)]].set(jnp.asarray(lengths, jnp.int32))

    lengths = jnp.where(number % 4 == 0, named(crowded, number // 4), named(usual, number - number // 4 - 1))
    mixed = jax.random.permutation(jax.random.fold_in(own, 3), number_of)
    source_of, receiver = mixed[0:number_of // 2 * 2:2], mixed[1:number_of // 2 * 2:2]
    slack = jnp.minimum(lengths[source_of] - 1, limit - lengths[receiver]) // 2
    slack = jnp.where((source_of == order[0]) | (receiver == order[0]) | (lengths[receiver] == 0), 0, jnp.maximum(slack, 0))
    passed = jax.random.randint(jax.random.fold_in(own, 4), (number_of // 2,), 0, 1 << 20) % (slack + 1)
    lengths = lengths.at[source_of].add(-passed).at[receiver].add(passed)
    items = jnp.searchsorted(jnp.cumsum(lengths), jnp.arange(rows * top), side="right").astype(jnp.int32)
    listing = items.reshape(top, rows).T
    listing = listing[jax.random.permutation(jax.random.fold_in(own, 1), rows)]
    turn = jax.random.randint(jax.random.fold_in(own, 2), (rows, 1), 0, top)
    return jnp.take_along_axis(listing, (jnp.arange(top)[None, :] + turn) % top, axis=1)


def load_shares(amount, total, limit, skew, full):
    portions = [(1 << 20) // math.isqrt(grade ** skew) + 1 for grade in range(1, amount + 1)]
    largest = limit if full else min(limit, max(-(-total // amount), total * portions[0] // sum(portions)))
    least = 1 if total - largest >= amount - 1 else 0
    counts, rest = [largest] + [least] * (amount - 1), total - largest - least * (amount - 1)
    while rest > 0:
        movable = [i for i in range(1, amount) if counts[i] < largest] or [i for i in range(1, amount) if counts[i] < limit]
        mass, left = sum([portions[i] for i in movable]), rest
        for i in movable:
            more = min(limit - counts[i], max(1, left * portions[i] // mass), rest)
            counts[i] = counts[i] + more
            rest = rest - more
    return np.array(counts)


def gaussian(own_key, extent, width, limit, cuts=(), kind=jnp.bfloat16):
    gain = block_scale(own_key, extent, cuts, -0.22, 0.18) if cuts else 1.0
    entries = jax.random.normal(own_key, extent, jnp.float32) * width * gain
    return jnp.minimum(jnp.maximum(entries, -limit), limit).astype(kind)


def setup_inputs(seed: int = 0) -> dict:
    key_list = jax.random.split(jax.random.key(seed), 10)
    tokens = gaussian(key_list[0], (TOKENS, D), 1.0, 6.0, ((0, 64), (1, 4)))
    expert_ids_keys = jax.random.split(jax.random.fold_in(key_list[1], 1), TOKENS // TOK_DEV)
    expert_ids_turns = jax.random.permutation(jax.random.fold_in(key_list[1], 3), TOKENS // TOK_DEV)
    expert_ids = jax.vmap(lambda own, number: assign_block(jax.random.fold_in(key_list[1], 2), own, number, TOK_DEV, EXPERTS, TOPK, CAP, 2))(expert_ids_keys, expert_ids_turns).reshape((TOKENS, TOPK))
    gate_values = jnp.clip(0.049804688 + 0.3486328 * jax.random.uniform(key_list[2], (TOKENS, TOPK), jnp.float32) ** block_scale(key_list[2], (TOKENS, TOPK), ((0, 64),), -0.2, 0.2), 0.049804688, 0.3984375).astype(jnp.bfloat16)
    w_gate = gaussian(key_list[3], (EXPERTS, D, FF), D ** -0.5, 0.09375, ((0, 64), (2, 4)))
    w_up = gaussian(key_list[4], (EXPERTS, D, FF), D ** -0.5, 0.09375, ((0, 64), (2, 4)))
    w_down = gaussian(key_list[5], (EXPERTS, FF, D), FF ** -0.5, 0.1875, ((0, 64), (1, 4)))
    shared_gate = gaussian(key_list[6], (D, SFF), D ** -0.5, 0.09375, ((1, 4),))
    shared_up = gaussian(key_list[7], (D, SFF), D ** -0.5, 0.09375, ((1, 4),))
    shared_down = gaussian(key_list[8], (SFF, D), SFF ** -0.5, 0.1875, ((0, 4),))
    return dict(tokens=tokens, expert_ids=expert_ids, gate_values=gate_values, w_gate=w_gate, w_up=w_up, w_down=w_down, shared_gate=shared_gate, shared_up=shared_up, shared_down=shared_down)


def reference(tokens, expert_ids, gate_values, w_gate, w_up, w_down, shared_gate, shared_up, shared_down):
    block_count = TOKENS // TOK_DEV
    slot_rows = block_count * CAP
    quarter = FF // N_TENSOR
    numbers = jnp.arange(EXPERTS, dtype=jnp.int32)
    grouped = expert_ids.reshape(block_count, TOK_DEV, TOPK)
    onehot = (grouped[..., None] == numbers).astype(jnp.int32)
    per_token = jnp.sum(onehot, axis=2)
    earlier = jnp.cumsum(per_token, axis=1) - per_token
    slot_index = jnp.sum(onehot * earlier[:, :, None, :], axis=3)
    position = (jnp.arange(block_count, dtype=jnp.int32)[:, None, None] * CAP + slot_index).reshape(TOKENS, TOPK)
    token_index = jnp.arange(TOKENS, dtype=jnp.int32)
    padded = jnp.concatenate([tokens, jnp.zeros((1, D), tokens.dtype)], axis=0)
    gate_float = gate_values.astype(jnp.float32)

    def one_expert(combined, inputs):
        gate_matrix, up_matrix, down_matrix, number = inputs
        chosen = expert_ids == number
        location = jnp.sum(jnp.where(chosen, position, 0), axis=1).astype(jnp.int32)
        weight = jnp.sum(jnp.where(chosen, gate_float, 0.0), axis=1)
        used = jnp.any(chosen, axis=1)
        owners = jnp.full((slot_rows,), TOKENS, jnp.int32)
        owners = owners.at[jnp.where(used, location, slot_rows).astype(jnp.int32)].set(token_index, mode="drop")
        rows = padded[owners].astype(jnp.float32)
        gate_sums = jnp.dot(rows, gate_matrix.astype(jnp.float32), precision=lax.Precision.HIGHEST)
        up_sums = jnp.dot(rows, up_matrix.astype(jnp.float32), precision=lax.Precision.HIGHEST)
        hidden = (jax.nn.silu(gate_sums) * up_sums).astype(jnp.bfloat16)
        blocks = jnp.einsum("rqf,qfd->rqd", hidden.reshape(slot_rows, N_TENSOR, quarter).astype(jnp.float32),
                            down_matrix.reshape(N_TENSOR, quarter, D).astype(jnp.float32),
                            precision=lax.Precision.HIGHEST)
        rounded = lax.optimization_barrier(blocks.astype(jnp.bfloat16))
        expert_out = jnp.sum(rounded.astype(jnp.float32), axis=1)
        picked = expert_out[jnp.minimum(location, slot_rows - 1)]
        return combined + weight[:, None] * picked, None

    start = jnp.zeros((TOKENS, D), jnp.float32)
    routed, unused = lax.scan(one_expert, start, (w_gate, w_up, w_down, numbers))
    token_float = tokens.astype(jnp.float32)
    shared_hidden = (jax.nn.silu(jnp.dot(token_float, shared_gate.astype(jnp.float32), precision=lax.Precision.HIGHEST))
                     * jnp.dot(token_float, shared_up.astype(jnp.float32), precision=lax.Precision.HIGHEST)).astype(jnp.bfloat16)
    shared_out = jnp.dot(shared_hidden, shared_down, preferred_element_type=jnp.float32)
    return (routed + shared_out).astype(jnp.bfloat16)
```

```python
import jax
import jax.numpy as jnp
from jax import lax
from jax.experimental import pallas as pl
from jax.experimental.pallas import tpu as pltpu
from jax.sharding import Mesh
from jax.sharding import PartitionSpec as P

EXPERT = ("expert_0", "expert_1", "expert_2")
CHUNKS = (8, 4)
F32 = jnp.float32
BF16 = jnp.bfloat16


def dot(a, b):
    return jnp.dot(a, b, preferred_element_type=F32)


def silu_times(gate, up):
    return (gate / (1.0 + jnp.exp(-gate)) * up).astype(BF16)


def kernel_call(body, outs, *args, smem=0):
    specs = [pl.BlockSpec(memory_space=pltpu.SMEM) for _ in range(smem)]
    specs += [pl.BlockSpec(memory_space=pltpu.VMEM) for _ in args[smem:]]
    return pl.pallas_call(
        body,
        in_specs=specs,
        out_specs=tuple(pl.BlockSpec(memory_space=pltpu.VMEM) for _ in outs),
        out_shape=tuple(jax.ShapeDtypeStruct(*o) for o in outs),
    )(*args)


def route_body(experts):
    def body(ids_ref, gates_ref, tokens_ref, *outs):
        ids = ids_ref[...]
        gates = gates_ref[...].astype(F32)
        rows, top = ids.shape
        numbers = lax.broadcasted_iota(jnp.int32, (rows, experts), 1)
        named = [ids[:, k : k + 1] == numbers for k in range(top)]
        onehot = [jnp.where(n, 1.0, 0.0) for n in named]
        per_token = sum(onehot[1:], onehot[0])
        before = lax.broadcasted_iota(jnp.int32, (rows, rows), 0) > lax.broadcasted_iota(
            jnp.int32, (rows, rows), 1
        )
        earlier = dot(jnp.where(before, 1.0, 0.0).astype(BF16), per_token.astype(BF16))
        slots = [
            jnp.sum(o * earlier, axis=1, keepdims=True).astype(jnp.int32) for o in onehot
        ]
        first = 0
        for j, size in enumerate(CHUNKS):
            place = lax.broadcasted_iota(jnp.int32, (rows, experts * size), 1)
            pick = jnp.zeros((rows, experts * size), F32)
            weight = jnp.zeros((rows, experts * size), F32)
            for k in range(top):
                local = slots[k] - first
                inside = (local >= 0) & (local < size)
                target = jnp.where(inside, ids[:, k : k + 1] * size + local, -1)
                here = target == place
                pick = jnp.where(here, 1.0, pick)
                weight = jnp.where(here, gates[:, k : k + 1], weight)
            outs[2 * j][...] = lax.dot_general(
                pick.astype(BF16),
                tokens_ref[...],
                (((0,), (0,)), ((), ())),
                preferred_element_type=F32,
            ).astype(BF16)
            outs[2 * j + 1][...] = weight.astype(BF16)
            first += size

    return body


def shared_body(x_ref, gate_ref, up_ref, down_ref, out_ref):
    pieces = x_ref.shape[0]
    gate = sum(dot(x_ref[s], gate_ref[s]) for s in range(pieces))
    up = sum(dot(x_ref[s], up_ref[s]) for s in range(pieces))
    hidden = silu_times(gate, up)
    width = out_ref.shape[2]
    for s in range(pieces):
        out_ref[s] = dot(hidden, down_ref[:, s * width : (s + 1) * width]).astype(BF16)


def hidden_body(q_ref, own_ref, left_ref, right_ref, o0_ref, o1_ref, gate_ref, up_ref, out_ref):
    q = q_ref[0]
    n = gate_ref.shape[0]
    half = o0_ref.shape[0]
    for part in range(2):
        span = pl.ds(part * half, half)
        opposite = (o0_ref, o1_ref)[part]
        rows = ((own_ref[span], 0), (left_ref[span], n - 1), (right_ref[span], 1), (opposite[...], 2))
        gate = sum(dot(x, gate_ref[lax.rem(q + s, n)]) for x, s in rows)
        up = sum(dot(x, up_ref[lax.rem(q + s, n)]) for x, s in rows)
        out_ref[span] = silu_times(gate, up)


def down_body(h_ref, down_ref, out_ref):
    out_ref[...] = sum(dot(h_ref[s], down_ref[s]) for s in range(h_ref.shape[0])).astype(BF16)


def combine_body(*refs):
    count = len(CHUNKS)
    parts_ref, out_ref = refs[2 * count :]
    total = sum(parts_ref[s].astype(F32) for s in range(parts_ref.shape[0]))
    for j in range(count):
        total = total + dot(refs[2 * j][...], refs[2 * j + 1][...])
    out_ref[...] = total.astype(BF16)


def exchange(x, axis):
    return lax.all_to_all(x, axis, split_axis=0, concat_axis=0, tiled=True)


def to_all(x, axis):
    return exchange(jnp.broadcast_to(x, (lax.axis_size(axis), *x.shape)), axis)


def shift(x, axis, by):
    n = lax.axis_size(axis)
    return lax.ppermute(x, axis, [(i, (i + by) % n) for i in range(n)])


def per_device(
    tokens, expert_ids, gate_values, w_gate, w_up, w_down, shared_gate, shared_up, shared_down
):
    tok_dev, narrow = tokens.shape
    _, features, quarter = w_gate.shape
    experts = lax.axis_size(EXPERT)
    n = lax.axis_size("tensor")
    q = lax.axis_index("tensor").reshape(1)

    tokens_all = to_all(tokens, "tensor")
    routed = kernel_call(
        route_body(experts),
        [
            o
            for size in CHUNKS
            for o in (((experts * size, narrow), BF16), ((tok_dev, experts * size), BF16))
        ],
        expert_ids,
        gate_values,
        tokens,
    )
    weights = routed[1::2]
    arrived = [
        exchange(rows.reshape(experts, size, narrow), EXPERT).reshape(-1, narrow)
        for rows, size in zip(routed[0::2], CHUNKS)
    ]
    down = exchange(jnp.moveaxis(w_down.reshape(quarter, n, narrow), 1, 0), "tensor")

    shared_parts = kernel_call(
        shared_body,
        [((n, tok_dev, narrow), BF16)],
        tokens_all,
        shared_gate.reshape(n, narrow, -1),
        shared_up.reshape(n, narrow, -1),
        shared_down,
    )[0]

    returned = []
    for rows, size in zip(arrived, CHUNKS):
        half = rows.shape[0] // 2
        left = shift(rows, "tensor", 1)
        right = shift(rows, "tensor", -1)
        o0 = shift(left[:half], "tensor", 1)
        o1 = shift(right[half:], "tensor", -1)
        hidden = kernel_call(
            hidden_body,
            [((rows.shape[0], quarter), BF16)],
            q,
            rows,
            left,
            right,
            o0,
            o1,
            w_gate.reshape(n, narrow, quarter),
            w_up.reshape(n, narrow, quarter),
            smem=1,
        )[0]
        hidden_all = to_all(hidden, "tensor")
        out = kernel_call(down_body, [((rows.shape[0], narrow), BF16)], hidden_all, down)[0]
        returned.append(exchange(out.reshape(experts, size, narrow), EXPERT).reshape(-1, narrow))
    shared_all = exchange(shared_parts, "tensor")
    pairs = [a for pair in zip(weights, returned) for a in pair]
    return kernel_call(combine_body, [((tok_dev, narrow), BF16)], *pairs, shared_all)[0]


def solution(mesh):
    torus = Mesh(
        mesh.devices.reshape(4, 8, 2, mesh.shape["tensor"]),
        ("expert_0", "expert_1", "expert_2", "tensor"),
    )
    placed = (
        P(EXPERT, "tensor"),
        P(EXPERT, None),
        P(EXPERT, None),
        P(EXPERT, None, "tensor"),
        P(EXPERT, None, "tensor"),
        P(EXPERT, "tensor", None),
        P(None, "tensor"),
        P(None, "tensor"),
        P("tensor", None),
    )
    return jax.shard_map(
        per_device, mesh=torus, in_specs=placed, out_specs=P(EXPERT, "tensor"), check_vma=False
    )
```

```python
import jax
import jax.numpy as jnp
from jax import lax
from jax.experimental import pallas as pl
from jax.experimental.pallas import tpu as pltpu
from jax.sharding import Mesh
from jax.sharding import PartitionSpec as P

EXPERT = ("expert_0", "expert_1", "expert_2")
CHUNKS = (4, 4, 4)
TURNS = (0, 3, 1, 2)
F32 = jnp.float32
BF16 = jnp.bfloat16


def dot(a, b):
    return jnp.dot(a, b, preferred_element_type=F32)


def flat(ref):
    x = ref[...]
    return x.reshape(-1, x.shape[-1])


def silu_times(gate, up):
    return (gate / (1.0 + jnp.exp(-gate)) * up).astype(BF16)


def kernel_call(body, outs, *args, smem=0, vmem=16, flops=1):
    specs = [pl.BlockSpec(memory_space=pltpu.SMEM) for _ in range(smem)]
    specs += [pl.BlockSpec(memory_space=pltpu.VMEM) for _ in args[smem:]]
    return pl.pallas_call(
        body,
        in_specs=specs,
        out_specs=[pl.BlockSpec(memory_space=pltpu.VMEM) for _ in outs],
        out_shape=[jax.ShapeDtypeStruct(o, BF16) for o in outs],
        compiler_params=pltpu.CompilerParams(vmem_limit_bytes=vmem << 20),
        cost_estimate=pl.CostEstimate(flops=flops, transcendentals=0, bytes_accessed=0),
    )(*args)


def block(ref, index, width):
    return ref[:, pl.ds(pl.multiple_of(index * width, 128), width)]


def columns_body(q_ref, x_ref, *outs):
    n = len(outs)
    for s, out_ref in enumerate(outs):
        out_ref[...] = block(x_ref, lax.rem(q_ref[0] + s, n), out_ref.shape[1])


def gather_body(experts, first):
    def body(ids_ref, tokens_ref, out_ref):
        ids = ids_ref[...]
        top, rows = ids.shape
        size = out_ref.shape[1]
        numbers = lax.broadcasted_iota(jnp.int32, (experts, rows), 0)
        onehot = [jnp.where(ids[k : k + 1] == numbers, 1.0, 0.0) for k in range(top)]
        per_token = sum(onehot[1:], onehot[0])
        before = lax.broadcasted_iota(jnp.int32, (rows, rows), 0) < lax.broadcasted_iota(
            jnp.int32, (rows, rows), 1
        )
        earlier = dot(per_token.astype(BF16), jnp.where(before, 1.0, 0.0).astype(BF16))
        place = lax.broadcasted_iota(jnp.int32, (experts * size, rows), 0)
        pick = jnp.zeros((experts * size, rows), F32)
        for k in range(top):
            slot = jnp.sum(onehot[k] * earlier, axis=0, keepdims=True).astype(jnp.int32)
            local = slot - first
            inside = (local >= 0) & (local < size)
            target = jnp.where(inside, ids[k : k + 1] * size + local, -1)
            pick = jnp.where(target == place, 1.0, pick)
        out_ref[...] = dot(pick.astype(BF16), tokens_ref[...]).astype(BF16).reshape(out_ref.shape)

    return body


def weight_body(experts):
    def body(ids_ref, gates_ref, out_ref):
        ids = ids_ref[...]
        gates = gates_ref[...].astype(F32)
        rows, top = ids.shape
        numbers = lax.broadcasted_iota(jnp.int32, (rows, experts), 1)
        onehot = [jnp.where(ids[:, k : k + 1] == numbers, 1.0, 0.0) for k in range(top)]
        per_token = sum(onehot[1:], onehot[0])
        before = lax.broadcasted_iota(jnp.int32, (rows, rows), 0) > lax.broadcasted_iota(
            jnp.int32, (rows, rows), 1
        )
        earlier = dot(jnp.where(before, 1.0, 0.0).astype(BF16), per_token.astype(BF16))
        slots = [
            jnp.sum(o * earlier, axis=1, keepdims=True).astype(jnp.int32) for o in onehot
        ]
        first = start = 0
        for size in CHUNKS:
            width = experts * size
            place = lax.broadcasted_iota(jnp.int32, (rows, width), 1)
            weight = jnp.zeros((rows, width), F32)
            for k in range(top):
                local = slots[k] - first
                inside = (local >= 0) & (local < size)
                target = jnp.where(inside, ids[:, k : k + 1] * size + local, -1)
                weight = jnp.where(target == place, gates[:, k : k + 1], weight)
            out_ref[:, start : start + width] = weight.astype(BF16)
            first += size
            start += width

    return body


def matmul_halves(q_ref, xs, gate_ref, up_ref):
    n = gate_ref.shape[0]
    at = [lax.rem(q_ref[0] + s, n) for s in TURNS]
    gate = sum(dot(x, gate_ref[i]) for x, i in zip(xs, at))
    up = sum(dot(x, up_ref[i]) for x, i in zip(xs, at))
    return silu_times(gate, up)


def shared_body(q_ref, *refs):
    n = len(TURNS)
    gate_ref, up_ref, down_ref = refs[n : n + 3]
    outs = refs[n + 3 :]
    hidden = matmul_halves(q_ref, [r[...] for r in refs[:n]], gate_ref, up_ref)
    for s, out_ref in enumerate(outs):
        part = block(down_ref, lax.rem(q_ref[0] + s, n), out_ref.shape[1])
        out_ref[...] = dot(hidden, part).astype(BF16)


def hidden_body(q_ref, *refs):
    n = len(TURNS)
    gate_ref, up_ref, out_ref = refs[n:]
    out_ref[...] = matmul_halves(q_ref, [flat(r) for r in refs[:n]], gate_ref, up_ref)


def down_body(*refs):
    *ins, out_ref = refs
    n = len(TURNS)
    total = sum(dot(h[...], w[...]) for h, w in zip(ins[:n], ins[n:]))
    out_ref[...] = total.astype(BF16).reshape(out_ref.shape)


def combine_body(weight_ref, *refs):
    *ins, out_ref = refs
    rows_refs, parts = ins[: len(CHUNKS)], ins[len(CHUNKS) :]
    total = sum(p[...].astype(F32) for p in parts)
    start = 0
    for rows_ref in rows_refs:
        rows = flat(rows_ref)
        total = total + dot(weight_ref[:, start : start + rows.shape[0]], rows)
        start += rows.shape[0]
    out_ref[...] = total.astype(BF16)


def exchange(x, axis):
    return lax.all_to_all(x, axis, split_axis=0, concat_axis=0, tiled=True)


def shift(x, axis, by):
    n = lax.axis_size(axis)
    return lax.ppermute(x, axis, [(i, (i + by) % n) for i in range(n)])


def spread(x):
    return [x, shift(x, "tensor", 1), shift(x, "tensor", -1), shift(x, "tensor", 2)]


def deal(xs):
    return [xs[0], shift(xs[1], "tensor", 1), shift(xs[3], "tensor", -1), shift(xs[2], "tensor", 2)]


def ring(x, turn):
    left = shift(x, "tensor", 1)
    right = shift(x, "tensor", -1)
    return [x, left, right, shift(left if turn == 1 else right, "tensor", turn)]


def per_device(tokens, expert_ids, gate_values, w_gate, w_up, w_down, *shared):
    return layer(tokens, expert_ids, gate_values, w_gate, w_up, w_down[0], *shared)


def layer(
    tokens, expert_ids, gate_values, w_gate, w_up, w_down, shared_gate, shared_up, shared_down
):
    tok_dev, narrow = tokens.shape
    _, _, quarter = w_gate.shape
    experts = lax.axis_size(EXPERT)
    n = lax.axis_size("tensor")
    q = lax.axis_index("tensor").reshape(1)
    w_gate = w_gate.reshape(n, narrow, quarter)
    w_up = w_up.reshape(n, narrow, quarter)

    ids_t = expert_ids.T
    arrived = []
    for j, size in enumerate(CHUNKS):
        (rows,) = kernel_call(
            gather_body(experts, sum(CHUNKS[:j])), [(experts, size, narrow)], ids_t, tokens
        )
        arrived.append(exchange(rows, EXPERT))
    tokens_all = spread(tokens)
    columns = kernel_call(columns_body, [(quarter, narrow)] * n, q, w_down, smem=1)
    down = deal(columns)
    (weight,) = kernel_call(
        weight_body(experts), [(tok_dev, experts * sum(CHUNKS))], expert_ids, gate_values
    )
    shared_parts = kernel_call(
        shared_body,
        [(tok_dev, narrow)] * n,
        q,
        *tokens_all,
        shared_gate.reshape(n, narrow, -1),
        shared_up.reshape(n, narrow, -1),
        shared_down,
        smem=1,
        flops=10**9,
    )

    returned = []
    for j, (rows, size) in enumerate(zip(arrived, CHUNKS)):
        rows_all = ring(rows, 1 - 2 * (j % 2))
        (hidden,) = kernel_call(
            hidden_body,
            [(experts * size, quarter)],
            q,
            *rows_all,
            w_gate,
            w_up,
            smem=1,
            flops=10**9,
        )
        hidden_all = spread(hidden)
        (out,) = kernel_call(down_body, [(experts, size, narrow)], *hidden_all, *down, flops=10**9)
        returned.append(exchange(out, EXPERT))
    shared_all = deal(shared_parts)
    return kernel_call(combine_body, [(tok_dev, narrow)], weight, *returned, *shared_all)[0]


def solution(mesh):
    torus = Mesh(
        mesh.devices.reshape(4, 8, 2, mesh.shape["tensor"]),
        ("expert_0", "expert_1", "expert_2", "tensor"),
    )
    placed = (
        P(EXPERT, "tensor"),
        P(EXPERT, None),
        P(EXPERT, None),
        P(EXPERT, None, "tensor"),
        P(EXPERT, None, "tensor"),
        P(EXPERT, "tensor", None),
        P(None, "tensor"),
        P(None, "tensor"),
        P("tensor", None),
    )
    return jax.shard_map(
        per_device, mesh=torus, in_specs=placed, out_specs=P(EXPERT, "tensor"), check_vma=False
    )
```

```python
import jax
import jax.numpy as jnp
from jax import lax
from jax.experimental import pallas as pl
from jax.experimental.pallas import tpu as pltpu
from jax.sharding import Mesh
from jax.sharding import PartitionSpec as P

EXPERT = ("expert_0", "expert_1", "expert_2")
CHUNKS = (6, 6)
PAIR = 2
TURNS = (0, 3, 1, 2)
F32 = jnp.float32
BF16 = jnp.bfloat16


def dot(a, b):
    return jnp.dot(a, b, preferred_element_type=F32)


def flat(ref, width):
    x = ref[...]
    count = x.shape[2] // width
    parts = [x[:, :, p * width : (p + 1) * width].reshape(-1, width) for p in range(count)]
    return jnp.concatenate(parts, axis=0)


def unflat(out_ref, x):
    width = x.shape[1]
    count = out_ref.shape[2] // width
    rows = x.shape[0] // count
    for p in range(count):
        part = x[p * rows : (p + 1) * rows]
        out_ref[:, :, p * width : (p + 1) * width] = part.reshape(-1, PAIR, width)


def silu_times(gate, up):
    return (gate / (1.0 + jnp.exp(-gate)) * up).astype(BF16)


def kernel_call(body, outs, *args, smem=0, hbm=0, scratch=(), vmem=16, flops=1):
    places = [pltpu.SMEM] * smem + [pltpu.VMEM] * (len(args) - smem - hbm) + [pltpu.HBM] * hbm
    return pl.pallas_call(
        body,
        in_specs=[pl.BlockSpec(memory_space=m) for m in places],
        out_specs=[pl.BlockSpec(memory_space=pltpu.VMEM) for _ in outs],
        out_shape=[jax.ShapeDtypeStruct(o, BF16) for o in outs],
        scratch_shapes=scratch,
        compiler_params=pltpu.CompilerParams(vmem_limit_bytes=vmem << 20),
        cost_estimate=pl.CostEstimate(flops=flops, transcendentals=0, bytes_accessed=0),
    )(*args)


def block(ref, index, width):
    return ref[:, pl.ds(pl.multiple_of(index * width, 128), width)]


def columns_body(q_ref, x_ref, *outs):
    n = len(outs)
    for s, out_ref in enumerate(outs):
        out_ref[...] = block(x_ref, lax.rem(q_ref[0] + s, n), out_ref.shape[1])


def gather_body(experts, first, size):
    def body(ids_ref, tokens_ref, out_ref):
        ids = ids_ref[...]
        top, rows = ids.shape
        numbers = lax.broadcasted_iota(jnp.int32, (experts, rows), 0)
        onehot = [jnp.where(ids[k : k + 1] == numbers, 1.0, 0.0) for k in range(top)]
        per_token = sum(onehot[1:], onehot[0])
        before = lax.broadcasted_iota(jnp.int32, (rows, rows), 0) < lax.broadcasted_iota(
            jnp.int32, (rows, rows), 1
        )
        earlier = dot(per_token.astype(BF16), jnp.where(before, 1.0, 0.0).astype(BF16))
        slots = [
            jnp.sum(o * earlier, axis=0, keepdims=True).astype(jnp.int32) for o in onehot
        ]
        place = lax.broadcasted_iota(jnp.int32, (experts * PAIR, rows), 0)
        picks = []
        for p in range(first, first + size, PAIR):
            pick = jnp.zeros((experts * PAIR, rows), F32)
            for k in range(top):
                local = slots[k] - p
                inside = (local >= 0) & (local < PAIR)
                target = jnp.where(inside, ids[k : k + 1] * PAIR + local, -1)
                pick = jnp.where(target == place, 1.0, pick)
            picks.append(pick.astype(BF16))
        unflat(out_ref, dot(jnp.concatenate(picks, axis=0), tokens_ref[...]).astype(BF16))

    return body


def weight_body(experts):
    def body(ids_ref, gates_ref, out_ref):
        ids = ids_ref[...]
        gates = gates_ref[...].astype(F32)
        rows, top = ids.shape
        numbers = lax.broadcasted_iota(jnp.int32, (rows, experts), 1)
        onehot = [jnp.where(ids[:, k : k + 1] == numbers, 1.0, 0.0) for k in range(top)]
        per_token = sum(onehot[1:], onehot[0])
        before = lax.broadcasted_iota(jnp.int32, (rows, rows), 0) > lax.broadcasted_iota(
            jnp.int32, (rows, rows), 1
        )
        earlier = dot(jnp.where(before, 1.0, 0.0).astype(BF16), per_token.astype(BF16))
        slots = [
            jnp.sum(o * earlier, axis=1, keepdims=True).astype(jnp.int32) for o in onehot
        ]
        width = experts * PAIR
        place = lax.broadcasted_iota(jnp.int32, (rows, width), 1)
        for i in range(sum(CHUNKS) // PAIR):
            weight = jnp.zeros((rows, width), F32)
            for k in range(top):
                local = slots[k] - i * PAIR
                inside = (local >= 0) & (local < PAIR)
                target = jnp.where(inside, ids[:, k : k + 1] * PAIR + local, -1)
                weight = jnp.where(target == place, gates[:, k : k + 1], weight)
            out_ref[:, i * width : (i + 1) * width] = weight.astype(BF16)

    return body


def matmul_halves(q_ref, xs, gate_ref, up_ref):
    n = gate_ref.shape[0]
    at = [lax.rem(q_ref[0] + s, n) for s in TURNS]
    gate = sum(dot(x, gate_ref[i]) for x, i in zip(xs, at))
    up = sum(dot(x, up_ref[i]) for x, i in zip(xs, at))
    return silu_times(gate, up)


def shared_body(q_ref, *refs):
    n = len(TURNS)
    gate_ref, up_ref, down_ref = refs[n : n + 3]
    outs = refs[n + 3 :]
    hidden = matmul_halves(q_ref, [r[...] for r in refs[:n]], gate_ref, up_ref)
    for s, out_ref in enumerate(outs):
        part = block(down_ref, lax.rem(q_ref[0] + s, n), out_ref.shape[1])
        out_ref[...] = dot(hidden, part).astype(BF16)


def hidden_body(q_ref, *refs):
    n = len(TURNS)
    gate_hbm, up_hbm, out_ref, gate_ref, up_ref, sems = refs[n:]
    width = gate_ref.shape[1]
    at = [lax.rem(q_ref[0] + s, n) for s in TURNS]
    copies = []
    for i in range(n):
        pair = (
            pltpu.make_async_copy(gate_hbm.at[at[i]], gate_ref.at[i], sems.at[i, 0]),
            pltpu.make_async_copy(up_hbm.at[at[i]], up_ref.at[i], sems.at[i, 1]),
        )
        for c in pair:
            c.start()
        copies.append(pair)
    gate = up = 0.0
    for i in range(n):
        x = flat(refs[i], width)
        for c in copies[i]:
            c.wait()
        gate = gate + dot(x, gate_ref[i])
        up = up + dot(x, up_ref[i])
    out_ref[...] = silu_times(gate, up)


def down_body(*refs):
    *ins, out_ref = refs
    n = len(TURNS)
    total = sum(dot(h[...], w[...]) for h, w in zip(ins[:n], ins[n:]))
    unflat(out_ref, total.astype(BF16))


def combine_body(weight_ref, *refs):
    *ins, out_ref = refs
    rows_refs, parts = ins[: len(CHUNKS)], ins[len(CHUNKS) :]
    total = sum(p[...].astype(F32) for p in parts)
    start = 0
    for rows_ref in rows_refs:
        rows = flat(rows_ref, out_ref.shape[1])
        total = total + dot(weight_ref[:, start : start + rows.shape[0]], rows)
        start += rows.shape[0]
    out_ref[...] = total.astype(BF16)


def exchange(x, axis):
    return lax.all_to_all(x, axis, split_axis=0, concat_axis=0, tiled=True)


def shift(x, axis, by):
    n = lax.axis_size(axis)
    return lax.ppermute(x, axis, [(i, (i + by) % n) for i in range(n)])


def spread(x):
    return [x, shift(x, "tensor", 1), shift(x, "tensor", -1), shift(x, "tensor", 2)]


def deal(xs):
    return [xs[0], shift(xs[1], "tensor", 1), shift(xs[3], "tensor", -1), shift(xs[2], "tensor", 2)]


def ring(x, turn):
    left = shift(x, "tensor", 1)
    right = shift(x, "tensor", -1)
    return [x, left, right, shift(left if turn == 1 else right, "tensor", turn)]


def per_device(tokens, expert_ids, gate_values, w_gate, w_up, w_down, *shared):
    return layer(tokens, expert_ids, gate_values, w_gate, w_up, w_down[0], *shared)


def layer(
    tokens, expert_ids, gate_values, w_gate, w_up, w_down, shared_gate, shared_up, shared_down
):
    tok_dev, narrow = tokens.shape
    _, _, quarter = w_gate.shape
    experts = lax.axis_size(EXPERT)
    n = lax.axis_size("tensor")
    q = lax.axis_index("tensor").reshape(1)
    w_gate = w_gate.reshape(n, narrow, quarter)
    w_up = w_up.reshape(n, narrow, quarter)

    ids_t = expert_ids.T
    tokens_all = spread(tokens)
    arrived = []
    for j, size in enumerate(CHUNKS):
        (rows,) = kernel_call(
            gather_body(experts, sum(CHUNKS[:j]), size),
            [(experts, PAIR, size // PAIR * narrow)],
            ids_t,
            tokens,
        )
        arrived.append(exchange(rows, EXPERT))
    columns = kernel_call(columns_body, [(quarter, narrow)] * n, q, w_down, smem=1)
    down = deal(columns)
    (weight,) = kernel_call(
        weight_body(experts), [(tok_dev, experts * sum(CHUNKS))], expert_ids, gate_values
    )
    shared_parts = kernel_call(
        shared_body,
        [(tok_dev, narrow)] * n,
        q,
        *tokens_all,
        shared_gate.reshape(n, narrow, -1),
        shared_up.reshape(n, narrow, -1),
        shared_down,
        smem=1,
        flops=10**9,
    )

    returned = []
    for j, (rows, size) in enumerate(zip(arrived, CHUNKS)):
        rows_all = ring(rows, 1 - 2 * (j % 2))
        (hidden,) = kernel_call(
            hidden_body,
            [(experts * size, quarter)],
            q,
            *rows_all,
            w_gate,
            w_up,
            smem=1,
            hbm=2,
            scratch=[
                pltpu.VMEM((n, narrow, quarter), BF16),
                pltpu.VMEM((n, narrow, quarter), BF16),
                pltpu.SemaphoreType.DMA((n, 2)),
            ],
            vmem=24,
            flops=10**9,
        )
        hidden_all = spread(hidden)
        (out,) = kernel_call(
            down_body, [(experts, PAIR, size // PAIR * narrow)], *hidden_all, *down, flops=10**9
        )
        returned.append(exchange(out, EXPERT))
    shared_all = deal(shared_parts)
    return kernel_call(combine_body, [(tok_dev, narrow)], weight, *returned, *shared_all)[0]


def solution(mesh):
    torus = Mesh(
        mesh.devices.reshape(4, 8, 2, mesh.shape["tensor"]),
        ("expert_0", "expert_1", "expert_2", "tensor"),
    )
    placed = (
        P(EXPERT, "tensor"),
        P(EXPERT, None),
        P(EXPERT, None),
        P(EXPERT, None, "tensor"),
        P(EXPERT, None, "tensor"),
        P(EXPERT, "tensor", None),
        P(None, "tensor"),
        P(None, "tensor"),
        P("tensor", None),
    )
    return jax.shard_map(
        per_device, mesh=torus, in_specs=placed, out_specs=P(EXPERT, "tensor"), check_vma=False
    )
```

```python
import jax
import jax.numpy as jnp
from jax import lax
from jax.experimental import pallas as pl
from jax.experimental.pallas import tpu as pltpu
from jax.sharding import Mesh
from jax.sharding import PartitionSpec as P

EXPERT = ("expert_0", "expert_1", "expert_2")
CHUNKS = (6, 6)
PAIR = 2
TURNS = (0, 3, 1, 2)
F32 = jnp.float32
BF16 = jnp.bfloat16


def dot(a, b):
    return jnp.dot(a, b, preferred_element_type=F32)


def flat(x, width):
    count = x.shape[2] // width
    parts = [x[:, :, p * width : (p + 1) * width].reshape(-1, width) for p in range(count)]
    return jnp.concatenate(parts, axis=0)


def unflat(out_ref, x, start=0):
    width = x.shape[1]
    count = out_ref.shape[2] // width
    rows = x.shape[0] // count
    span = pl.ds(start, rows // PAIR)
    for p in range(count):
        part = x[p * rows : (p + 1) * rows]
        out_ref[span, :, p * width : (p + 1) * width] = part.reshape(-1, PAIR, width)


def silu_times(gate, up):
    return (gate / (1.0 + jnp.exp(-gate)) * up).astype(BF16)


def kernel_call(body, outs, *args, smem=0, vmem=12, flops=1):
    places = [pltpu.SMEM] * smem + [pltpu.VMEM] * (len(args) - smem)
    return pl.pallas_call(
        body,
        in_specs=[pl.BlockSpec(memory_space=m) for m in places],
        out_specs=[pl.BlockSpec(memory_space=pltpu.VMEM) for _ in outs],
        out_shape=[
            o if isinstance(o, jax.ShapeDtypeStruct) else jax.ShapeDtypeStruct(o, BF16)
            for o in outs
        ],
        compiler_params=pltpu.CompilerParams(vmem_limit_bytes=vmem << 20),
        cost_estimate=pl.CostEstimate(flops=flops, transcendentals=0, bytes_accessed=0),
    )(*args)


def block(ref, index, width):
    return ref[:, pl.ds(pl.multiple_of(index * width, 128), width)]


def columns_body(q_ref, x_ref, *outs):
    n = len(outs)
    for s, out_ref in enumerate(outs):
        out_ref[...] = block(x_ref, lax.rem(q_ref[0] + s, n), out_ref.shape[1])


def gather_body(experts, first, size):
    def body(ids_ref, tokens_ref, out_ref):
        ids = ids_ref[...]
        top, rows = ids.shape
        numbers = lax.broadcasted_iota(jnp.int32, (experts, rows), 0)
        onehot = [jnp.where(ids[k : k + 1] == numbers, 1.0, 0.0) for k in range(top)]
        per_token = sum(onehot[1:], onehot[0])
        before = lax.broadcasted_iota(jnp.int32, (rows, rows), 0) < lax.broadcasted_iota(
            jnp.int32, (rows, rows), 1
        )
        earlier = dot(per_token.astype(BF16), jnp.where(before, 1.0, 0.0).astype(BF16))
        slots = [
            jnp.sum(o * earlier, axis=0, keepdims=True).astype(jnp.int32) for o in onehot
        ]
        place = lax.broadcasted_iota(jnp.int32, (experts * PAIR, rows), 0)
        picks = []
        for p in range(first, first + size, PAIR):
            pick = jnp.zeros((experts * PAIR, rows), F32)
            for k in range(top):
                local = slots[k] - p
                inside = (local >= 0) & (local < PAIR)
                target = jnp.where(inside, ids[k : k + 1] * PAIR + local, -1)
                pick = jnp.where(target == place, 1.0, pick)
            picks.append(pick.astype(BF16))
        unflat(out_ref, dot(jnp.concatenate(picks, axis=0), tokens_ref[...]).astype(BF16))

    return body


def weight_body(experts):
    def body(ids_ref, gates_ref, out_ref):
        ids = ids_ref[...]
        gates = gates_ref[...].astype(F32)
        rows, top = ids.shape
        numbers = lax.broadcasted_iota(jnp.int32, (rows, experts), 1)
        onehot = [jnp.where(ids[:, k : k + 1] == numbers, 1.0, 0.0) for k in range(top)]
        per_token = sum(onehot[1:], onehot[0])
        before = lax.broadcasted_iota(jnp.int32, (rows, rows), 0) > lax.broadcasted_iota(
            jnp.int32, (rows, rows), 1
        )
        earlier = dot(jnp.where(before, 1.0, 0.0).astype(BF16), per_token.astype(BF16))
        slots = [
            jnp.sum(o * earlier, axis=1, keepdims=True).astype(jnp.int32) for o in onehot
        ]
        width = experts * PAIR
        place = lax.broadcasted_iota(jnp.int32, (rows, width), 1)
        for i in range(sum(CHUNKS) // PAIR):
            weight = jnp.zeros((rows, width), F32)
            for k in range(top):
                local = slots[k] - i * PAIR
                inside = (local >= 0) & (local < PAIR)
                target = jnp.where(inside, ids[:, k : k + 1] * PAIR + local, -1)
                weight = jnp.where(target == place, gates[:, k : k + 1], weight)
            out_ref[:, i * width : (i + 1) * width] = weight.astype(BF16)

    return body


def matmul_halves(q_ref, xs, gate_ref, up_ref):
    n = gate_ref.shape[0]
    at = [lax.rem(q_ref[0] + s, n) for s in TURNS]
    gate = sum(dot(x, gate_ref[i]) for x, i in zip(xs, at))
    up = sum(dot(x, up_ref[i]) for x, i in zip(xs, at))
    return silu_times(gate, up)


def shared_body(q_ref, *refs):
    n = len(TURNS)
    gate_ref, up_ref, down_ref = refs[n : n + 3]
    outs = refs[n + 3 :]
    hidden = matmul_halves(q_ref, [r[...] for r in refs[:n]], gate_ref, up_ref)
    for s, out_ref in enumerate(outs):
        part = block(down_ref, lax.rem(q_ref[0] + s, n), out_ref.shape[1])
        out_ref[...] = dot(hidden, part).astype(BF16)


def partial_body(q_ref, own_ref, left_ref, right_ref, gate_ref, up_ref, sums_ref, far_ref):
    n, width, quarter = gate_ref.shape
    at = [lax.rem(q_ref[0] + s, n) for s in TURNS]
    half = own_ref.shape[0] // 2
    rows = sums_ref.shape[0] // 2
    for h in range(2):
        span = pl.ds(h * half, half)
        xs = [flat(r[span], width) for r in (own_ref, left_ref, right_ref)]
        out = pl.ds(h * rows, rows)
        sums_ref[out, :quarter] = sum(dot(x, gate_ref[i]) for x, i in zip(xs, at))
        sums_ref[out, quarter:] = sum(dot(x, up_ref[i]) for x, i in zip(xs, at))
    far_ref[0] = gate_ref[at[3]]
    far_ref[1] = up_ref[at[3]]


def hidden_body(sums_ref, o0_ref, o1_ref, far_ref, out_ref):
    _, width, quarter = far_ref.shape
    rows = sums_ref.shape[0] // 2
    for h, o_ref in enumerate((o0_ref, o1_ref)):
        span = pl.ds(h * rows, rows)
        x = flat(o_ref[...], width)
        gate = sums_ref[span, :quarter] + dot(x, far_ref[0])
        up = sums_ref[span, quarter:] + dot(x, far_ref[1])
        out_ref[span] = silu_times(gate, up)


def down_body(*refs):
    *ins, out_ref = refs
    n = len(TURNS)
    rows = ins[0].shape[0] // 2
    for h in range(2):
        span = pl.ds(h * rows, rows)
        total = sum(dot(a[span], w[...]) for a, w in zip(ins[:n], ins[n:]))
        unflat(out_ref, total.astype(BF16), h * out_ref.shape[0] // 2)


def combine_body(weight_ref, *refs):
    *ins, out_ref = refs
    rows_refs, parts = ins[: len(CHUNKS)], ins[len(CHUNKS) :]
    total = sum(p[...].astype(F32) for p in parts)
    start = 0
    for rows_ref in rows_refs:
        rows = flat(rows_ref[...], out_ref.shape[1])
        total = total + dot(weight_ref[:, start : start + rows.shape[0]], rows)
        start += rows.shape[0]
    out_ref[...] = total.astype(BF16)


def exchange(x, axis):
    return lax.all_to_all(x, axis, split_axis=0, concat_axis=0, tiled=True)


def shift(x, axis, by):
    n = lax.axis_size(axis)
    return lax.ppermute(x, axis, [(i, (i + by) % n) for i in range(n)])


def spread(x):
    return [x, shift(x, "tensor", 1), shift(x, "tensor", -1), shift(x, "tensor", 2)]


def deal(xs):
    return [xs[0], shift(xs[1], "tensor", 1), shift(xs[3], "tensor", -1), shift(xs[2], "tensor", 2)]


def ring(x):
    half = x.shape[0] // 2
    left = shift(x, "tensor", 1)
    right = shift(x, "tensor", -1)
    o0 = shift(left[:half], "tensor", 1)
    o1 = shift(right[half:], "tensor", -1)
    return left, right, o0, o1


def per_device(tokens, expert_ids, gate_values, w_gate, w_up, w_down, *shared):
    return layer(tokens, expert_ids, gate_values, w_gate, w_up, w_down[0], *shared)


def layer(
    tokens, expert_ids, gate_values, w_gate, w_up, w_down, shared_gate, shared_up, shared_down
):
    tok_dev, narrow = tokens.shape
    _, _, quarter = w_gate.shape
    experts = lax.axis_size(EXPERT)
    n = lax.axis_size("tensor")
    q = lax.axis_index("tensor").reshape(1)
    w_gate = w_gate.reshape(n, narrow, quarter)
    w_up = w_up.reshape(n, narrow, quarter)

    ids_t = expert_ids.T
    tokens_all = spread(tokens)
    arrived = []
    for j, size in enumerate(CHUNKS):
        (rows,) = kernel_call(
            gather_body(experts, sum(CHUNKS[:j]), size),
            [(experts, PAIR, size // PAIR * narrow)],
            ids_t,
            tokens,
        )
        arrived.append(exchange(rows, EXPERT))
    columns = kernel_call(columns_body, [(quarter, narrow)] * n, q, w_down, smem=1)
    down = deal(columns)
    (weight,) = kernel_call(
        weight_body(experts), [(tok_dev, experts * sum(CHUNKS))], expert_ids, gate_values
    )
    shared_parts = kernel_call(
        shared_body,
        [(tok_dev, narrow)] * n,
        q,
        *tokens_all,
        shared_gate.reshape(n, narrow, -1),
        shared_up.reshape(n, narrow, -1),
        shared_down,
        smem=1,
        flops=10**9,
    )

    returned = []
    for rows, size in zip(arrived, CHUNKS):
        left, right, o0, o1 = ring(rows)
        sums, far = kernel_call(
            partial_body,
            [
                jax.ShapeDtypeStruct((experts * size, 2 * quarter), F32),
                (2, narrow, quarter),
            ],
            q,
            rows,
            left,
            right,
            w_gate,
            w_up,
            smem=1,
            flops=10**9,
        )
        (hidden,) = kernel_call(
            hidden_body, [(experts * size, quarter)], sums, o0, o1, far, flops=10**9
        )
        hidden_all = spread(hidden)
        (out,) = kernel_call(
            down_body, [(experts, PAIR, size // PAIR * narrow)], *hidden_all, *down, flops=10**9
        )
        returned.append(exchange(out, EXPERT))
    shared_all = deal(shared_parts)
    return kernel_call(combine_body, [(tok_dev, narrow)], weight, *returned, *shared_all)[0]


def solution(mesh):
    torus = Mesh(
        mesh.devices.reshape(4, 8, 2, mesh.shape["tensor"]),
        ("expert_0", "expert_1", "expert_2", "tensor"),
    )
    placed = (
        P(EXPERT, "tensor"),
        P(EXPERT, None),
        P(EXPERT, None),
        P(EXPERT, None, "tensor"),
        P(EXPERT, None, "tensor"),
        P(EXPERT, "tensor", None),
        P(None, "tensor"),
        P(None, "tensor"),
        P("tensor", None),
    )
    return jax.shard_map(
        per_device, mesh=torus, in_specs=placed, out_specs=P(EXPERT, "tensor"), check_vma=False
    )
```

```python
import jax
import jax.numpy as jnp
from jax import lax
from jax.experimental import pallas as pl
from jax.experimental.pallas import tpu as pltpu
from jax.sharding import Mesh
from jax.sharding import PartitionSpec as P

EXPERT = ("expert_0", "expert_1", "expert_2")
CHUNKS = (6, 6)
PAIR = 2
TURNS = (0, 3, 1, 2)
F32 = jnp.float32
BF16 = jnp.bfloat16


def dot(a, b):
    return jnp.dot(a, b, preferred_element_type=F32)


def flat(x, width):
    count = x.shape[2] // width
    parts = [x[:, :, p * width : (p + 1) * width].reshape(-1, width) for p in range(count)]
    return jnp.concatenate(parts, axis=0)


def unflat(out_ref, x, lane=0):
    rows = out_ref.shape[0] * PAIR
    width = x.shape[1]
    for p in range(x.shape[0] // rows):
        part = x[p * rows : (p + 1) * rows].reshape(-1, PAIR, width)
        out_ref[:, :, lane + p * width : lane + (p + 1) * width] = part


def silu_times(gate, up):
    return (gate / (1.0 + jnp.exp(-gate)) * up).astype(BF16)


def kernel_call(body, outs, *args, smem=0, vmem=12, flops=1):
    places = [pltpu.SMEM] * smem + [pltpu.VMEM] * (len(args) - smem)
    return pl.pallas_call(
        body,
        in_specs=[pl.BlockSpec(memory_space=m) for m in places],
        out_specs=[pl.BlockSpec(memory_space=pltpu.VMEM) for _ in outs],
        out_shape=[
            o if isinstance(o, jax.ShapeDtypeStruct) else jax.ShapeDtypeStruct(o, BF16)
            for o in outs
        ],
        compiler_params=pltpu.CompilerParams(vmem_limit_bytes=vmem << 20),
        cost_estimate=pl.CostEstimate(flops=flops, transcendentals=0, bytes_accessed=0),
    )(*args)


def block(ref, index, width):
    return ref[:, pl.ds(pl.multiple_of(index * width, 128), width)]


def columns_body(q_ref, x_ref, *outs):
    n = len(outs)
    for s, out_ref in enumerate(outs):
        out_ref[...] = block(x_ref, lax.rem(q_ref[0] + s, n), out_ref.shape[1])


def gather_body(experts, first, size):
    def body(ids_ref, *refs):
        *tokens_refs, out_ref = refs
        ids = ids_ref[...]
        top, rows = ids.shape
        numbers = lax.broadcasted_iota(jnp.int32, (experts, rows), 0)
        onehot = [jnp.where(ids[k : k + 1] == numbers, 1.0, 0.0) for k in range(top)]
        per_token = sum(onehot[1:], onehot[0])
        before = lax.broadcasted_iota(jnp.int32, (rows, rows), 0) < lax.broadcasted_iota(
            jnp.int32, (rows, rows), 1
        )
        earlier = dot(per_token.astype(BF16), jnp.where(before, 1.0, 0.0).astype(BF16))
        slots = [
            jnp.sum(o * earlier, axis=0, keepdims=True).astype(jnp.int32) for o in onehot
        ]
        place = lax.broadcasted_iota(jnp.int32, (experts * PAIR, rows), 0)
        picks = []
        for p in range(first, first + size, PAIR):
            pick = jnp.zeros((experts * PAIR, rows), F32)
            for k in range(top):
                local = slots[k] - p
                inside = (local >= 0) & (local < PAIR)
                target = jnp.where(inside, ids[k : k + 1] * PAIR + local, -1)
                pick = jnp.where(target == place, 1.0, pick)
            picks.append(pick.astype(BF16))
        picks = jnp.concatenate(picks, axis=0)
        for s, tokens_ref in enumerate(tokens_refs):
            x = dot(picks, tokens_ref[...]).astype(BF16)
            unflat(out_ref, x, lane=s * (size // PAIR) * x.shape[1])

    return body


def weight_body(experts):
    def body(ids_ref, gates_ref, out_ref):
        ids = ids_ref[...]
        gates = gates_ref[...].astype(F32)
        rows, top = ids.shape
        numbers = lax.broadcasted_iota(jnp.int32, (rows, experts), 1)
        onehot = [jnp.where(ids[:, k : k + 1] == numbers, 1.0, 0.0) for k in range(top)]
        per_token = sum(onehot[1:], onehot[0])
        before = lax.broadcasted_iota(jnp.int32, (rows, rows), 0) > lax.broadcasted_iota(
            jnp.int32, (rows, rows), 1
        )
        earlier = dot(jnp.where(before, 1.0, 0.0).astype(BF16), per_token.astype(BF16))
        slots = [
            jnp.sum(o * earlier, axis=1, keepdims=True).astype(jnp.int32) for o in onehot
        ]
        width = experts * PAIR
        place = lax.broadcasted_iota(jnp.int32, (rows, width), 1)
        for i in range(sum(CHUNKS) // PAIR):
            weight = jnp.zeros((rows, width), F32)
            for k in range(top):
                local = slots[k] - i * PAIR
                inside = (local >= 0) & (local < PAIR)
                target = jnp.where(inside, ids[:, k : k + 1] * PAIR + local, -1)
                weight = jnp.where(target == place, gates[:, k : k + 1], weight)
            out_ref[:, i * width : (i + 1) * width] = weight.astype(BF16)

    return body


def matmul_halves(q_ref, xs, gate_ref, up_ref):
    n = gate_ref.shape[0]
    at = [lax.rem(q_ref[0] + s, n) for s in TURNS]
    gate = sum(dot(x, gate_ref[i]) for x, i in zip(xs, at))
    up = sum(dot(x, up_ref[i]) for x, i in zip(xs, at))
    return silu_times(gate, up)


def shared_body(q_ref, *refs):
    n = len(TURNS)
    gate_ref, up_ref, down_ref = refs[n : n + 3]
    outs = refs[n + 3 :]
    hidden = matmul_halves(q_ref, [r[...] for r in refs[:n]], gate_ref, up_ref)
    for s, out_ref in enumerate(outs):
        part = block(down_ref, lax.rem(q_ref[0] + s, n), out_ref.shape[1])
        out_ref[...] = dot(hidden, part).astype(BF16)


def ring_sums_body(q_ref, own_ref, left_ref, right_ref, gate_ref, up_ref, sums_ref, rest_ref):
    _, width, quarter = gate_ref.shape
    at = [lax.rem(q_ref[0] + s, len(TURNS)) for s in TURNS]
    half = own_ref.shape[0] // 2
    rows = sums_ref.shape[0] // 2
    for h in range(2):
        span = pl.ds(h * half, half)
        xs = [flat(r[span], width) for r in (own_ref, left_ref, right_ref)]
        out = pl.ds(h * rows, rows)
        sums_ref[out, :quarter] = sum(dot(x, gate_ref[i]) for x, i in zip(xs, at))
        sums_ref[out, quarter:] = sum(dot(x, up_ref[i]) for x, i in zip(xs, at))
    rest_ref[0] = gate_ref[at[3]]
    rest_ref[1] = up_ref[at[3]]


def ring_hidden_body(sums_ref, o0_ref, o1_ref, rest_ref, out_ref):
    _, width, quarter = rest_ref.shape
    x = jnp.concatenate([flat(o0_ref[...], width), flat(o1_ref[...], width)], axis=0)
    gate = sums_ref[:, :quarter] + dot(x, rest_ref[0])
    up = sums_ref[:, quarter:] + dot(x, rest_ref[1])
    out_ref[...] = silu_times(gate, up)


def pair_sums_body(q_ref, rows_ref, gate_ref, up_ref, sums_ref, rest_ref):
    _, width, quarter = gate_ref.shape
    at = [lax.rem(q_ref[0] + s, len(TURNS)) for s in TURNS]
    lanes = rows_ref.shape[2] // 2
    own = flat(rows_ref[:, :, :lanes], width)
    far = flat(rows_ref[:, :, lanes:], width)
    sums_ref[:, :quarter] = dot(own, gate_ref[at[0]]) + dot(far, gate_ref[at[3]])
    sums_ref[:, quarter:] = dot(own, up_ref[at[0]]) + dot(far, up_ref[at[3]])
    for i in range(2):
        rest_ref[2 * i] = gate_ref[at[1 + i]]
        rest_ref[2 * i + 1] = up_ref[at[1 + i]]


def pair_hidden_body(sums_ref, left_ref, right_ref, rest_ref, out_ref):
    _, width, quarter = rest_ref.shape
    left, right = flat(left_ref[...], width), flat(right_ref[...], width)
    gate = sums_ref[:, :quarter] + dot(left, rest_ref[0]) + dot(right, rest_ref[2])
    up = sums_ref[:, quarter:] + dot(left, rest_ref[1]) + dot(right, rest_ref[3])
    out_ref[...] = silu_times(gate, up)


def stack_body(*refs):
    *ins, out_ref = refs
    for s, ref in enumerate(ins):
        out_ref[s] = ref[...]


def down_body(halves):
    def body(*refs):
        *ins, down_ref, out_ref = refs
        count = out_ref.shape[0] // halves
        rows = ins[0].shape[0] // halves
        for h in range(halves):
            span = pl.ds(h * rows, rows)
            total = sum(dot(a[span], down_ref[s]) for s, a in enumerate(ins))
            unflat(out_ref.at[pl.ds(h * count, count)], total.astype(BF16))

    return body


def combine_body(weight_ref, *refs):
    *ins, out_ref = refs
    rows_refs, parts = ins[: len(CHUNKS)], ins[len(CHUNKS) :]
    total = sum(p[...].astype(F32) for p in parts)
    start = 0
    for rows_ref in rows_refs:
        rows = flat(rows_ref[...], out_ref.shape[1])
        total = total + dot(weight_ref[:, start : start + rows.shape[0]], rows)
        start += rows.shape[0]
    out_ref[...] = total.astype(BF16)


def exchange(x, axis):
    return lax.all_to_all(x, axis, split_axis=0, concat_axis=0, tiled=True)


def shift(x, axis, by):
    n = lax.axis_size(axis)
    return lax.ppermute(x, axis, [(i, (i + by) % n) for i in range(n)])


def spread(x):
    return [x, shift(x, "tensor", 1), shift(x, "tensor", -1), shift(x, "tensor", 2)]


def deal(xs):
    return [xs[0], shift(xs[1], "tensor", 1), shift(xs[3], "tensor", -1), shift(xs[2], "tensor", 2)]


def ring(x):
    half = x.shape[0] // 2
    left = shift(x, "tensor", 1)
    right = shift(x, "tensor", -1)
    o0 = shift(left[:half], "tensor", 1)
    o1 = shift(right[half:], "tensor", -1)
    return left, right, o0, o1


def per_device(tokens, expert_ids, gate_values, w_gate, w_up, w_down, *shared):
    return layer(tokens, expert_ids, gate_values, w_gate, w_up, w_down[0], *shared)


def layer(
    tokens, expert_ids, gate_values, w_gate, w_up, w_down, shared_gate, shared_up, shared_down
):
    tok_dev, narrow = tokens.shape
    _, _, quarter = w_gate.shape
    experts = lax.axis_size(EXPERT)
    n = lax.axis_size("tensor")
    q = lax.axis_index("tensor").reshape(1)
    w_gate = w_gate.reshape(n, narrow, quarter)
    w_up = w_up.reshape(n, narrow, quarter)

    ids_t = expert_ids.T
    tokens_all = spread(tokens)
    ids_t = expert_ids.T
    arrived = []
    for j, (size, sources) in enumerate(zip(CHUNKS, ([tokens], [tokens, tokens_all[3]]))):
        (rows,) = kernel_call(
            gather_body(experts, sum(CHUNKS[:j]), size),
            [(experts, PAIR, len(sources) * size // PAIR * narrow)],
            ids_t,
            *sources,
        )
        arrived.append(exchange(rows, EXPERT))
    columns = kernel_call(columns_body, [(quarter, narrow)] * n, q, w_down, smem=1)
    (down,) = kernel_call(stack_body, [(n, quarter, narrow)], *deal(columns))
    (weight,) = kernel_call(
        weight_body(experts), [(tok_dev, experts * sum(CHUNKS))], expert_ids, gate_values
    )
    shared_parts = kernel_call(
        shared_body,
        [(tok_dev, narrow)] * n,
        q,
        *tokens_all,
        shared_gate.reshape(n, narrow, -1),
        shared_up.reshape(n, narrow, -1),
        shared_down,
        smem=1,
        flops=10**9,
    )

    returned = []
    for j, (rows, size) in enumerate(zip(arrived, CHUNKS)):
        count = experts * size
        sums_shape = jax.ShapeDtypeStruct((count, 2 * quarter), F32)
        if j == 0:
            left, right, *last = ring(rows)
            args = (rows, left, right)
            bodies = ring_sums_body, ring_hidden_body
        else:
            own = rows[:, :, : size // PAIR * narrow]
            last = shift(own, "tensor", 1), shift(own, "tensor", -1)
            args = (rows,)
            bodies = pair_sums_body, pair_hidden_body
        sums, rest = kernel_call(
            bodies[0],
            [sums_shape, (2 * (1 + j), narrow, quarter)],
            q,
            *args,
            w_gate,
            w_up,
            smem=1,
            flops=10**9,
        )
        (hidden,) = kernel_call(bodies[1], [(count, quarter)], sums, *last, rest, flops=10**9)
        (out,) = kernel_call(
            down_body(2 - j),
            [(experts, PAIR, size // PAIR * narrow)],
            *spread(hidden),
            down,
            flops=10**9,
        )
        returned.append(exchange(out, EXPERT))
    shared_all = deal(shared_parts)
    return kernel_call(combine_body, [(tok_dev, narrow)], weight, *returned, *shared_all)[0]


def solution(mesh):
    torus = Mesh(
        mesh.devices.reshape(4, 8, 2, mesh.shape["tensor"]),
        ("expert_0", "expert_1", "expert_2", "tensor"),
    )
    placed = (
        P(EXPERT, "tensor"),
        P(EXPERT, None),
        P(EXPERT, None),
        P(EXPERT, None, "tensor"),
        P(EXPERT, None, "tensor"),
        P(EXPERT, "tensor", None),
        P(None, "tensor"),
        P(None, "tensor"),
        P("tensor", None),
    )
    return jax.shard_map(
        per_device, mesh=torus, in_specs=placed, out_specs=P(EXPERT, "tensor"), check_vma=False
    )
```

```python
import jax
import jax.numpy as jnp
from jax import lax
from jax.experimental import pallas as pl
from jax.experimental.pallas import tpu as pltpu
from jax.sharding import Mesh
from jax.sharding import PartitionSpec as P

EXPERT = ("expert_0", "expert_1", "expert_2")
CHUNKS = (6, 6)
PAIR = 2
TURNS = (0, 3, 1, 2)
F32 = jnp.float32
BF16 = jnp.bfloat16


def dot(a, b):
    return jnp.dot(a, b, preferred_element_type=F32)


def flat(x, width):
    count = x.shape[2] // width
    parts = [x[:, :, p * width : (p + 1) * width].reshape(-1, width) for p in range(count)]
    return jnp.concatenate(parts, axis=0)


def unflat(out_ref, x, lane=0):
    rows = out_ref.shape[0] * PAIR
    width = x.shape[1]
    for p in range(x.shape[0] // rows):
        part = x[p * rows : (p + 1) * rows].reshape(-1, PAIR, width)
        out_ref[:, :, lane + p * width : lane + (p + 1) * width] = part


def silu_times(gate, up):
    return (gate / (1.0 + jnp.exp(-gate)) * up).astype(BF16)


def kernel_call(body, outs, *args, smem=0, vmem=12, flops=1):
    places = [pltpu.SMEM] * smem + [pltpu.VMEM] * (len(args) - smem)
    return pl.pallas_call(
        body,
        in_specs=[pl.BlockSpec(memory_space=m) for m in places],
        out_specs=[pl.BlockSpec(memory_space=pltpu.VMEM) for _ in outs],
        out_shape=[
            o if isinstance(o, jax.ShapeDtypeStruct) else jax.ShapeDtypeStruct(o, BF16)
            for o in outs
        ],
        compiler_params=pltpu.CompilerParams(vmem_limit_bytes=vmem << 20),
        cost_estimate=pl.CostEstimate(flops=flops, transcendentals=0, bytes_accessed=0),
    )(*args)


def block(ref, index, width):
    return ref[:, pl.ds(pl.multiple_of(index * width, 128), width)]


def columns_body(q_ref, x_ref, *outs):
    n = len(outs)
    for s, out_ref in enumerate(outs):
        out_ref[...] = block(x_ref, lax.rem(q_ref[0] + s, n), out_ref.shape[1])


def gather_body(experts, first, size):
    def body(ids_ref, *refs):
        *tokens_refs, out_ref = refs
        ids = ids_ref[...]
        top, rows = ids.shape
        numbers = lax.broadcasted_iota(jnp.int32, (experts, rows), 0)
        onehot = [jnp.where(ids[k : k + 1] == numbers, 1.0, 0.0) for k in range(top)]
        per_token = sum(onehot[1:], onehot[0])
        before = lax.broadcasted_iota(jnp.int32, (rows, rows), 0) < lax.broadcasted_iota(
            jnp.int32, (rows, rows), 1
        )
        earlier = dot(per_token.astype(BF16), jnp.where(before, 1.0, 0.0).astype(BF16))
        slots = [
            jnp.sum(o * earlier, axis=0, keepdims=True).astype(jnp.int32) for o in onehot
        ]
        place = lax.broadcasted_iota(jnp.int32, (experts * PAIR, rows), 0)
        picks = []
        for p in range(first, first + size, PAIR):
            pick = jnp.zeros((experts * PAIR, rows), F32)
            for k in range(top):
                local = slots[k] - p
                inside = (local >= 0) & (local < PAIR)
                target = jnp.where(inside, ids[k : k + 1] * PAIR + local, -1)
                pick = jnp.where(target == place, 1.0, pick)
            picks.append(pick.astype(BF16))
        picks = jnp.concatenate(picks, axis=0)
        for s, tokens_ref in enumerate(tokens_refs):
            x = dot(picks, tokens_ref[...]).astype(BF16)
            unflat(out_ref, x, lane=s * (size // PAIR) * x.shape[1])

    return body


def weight_body(experts):
    def body(ids_ref, gates_ref, *outs):
        ids = ids_ref[...]
        gates = gates_ref[...].astype(F32)
        rows, top = ids.shape
        numbers = lax.broadcasted_iota(jnp.int32, (rows, experts), 1)
        onehot = [jnp.where(ids[:, k : k + 1] == numbers, 1.0, 0.0) for k in range(top)]
        per_token = sum(onehot[1:], onehot[0])
        before = lax.broadcasted_iota(jnp.int32, (rows, rows), 0) > lax.broadcasted_iota(
            jnp.int32, (rows, rows), 1
        )
        earlier = dot(jnp.where(before, 1.0, 0.0).astype(BF16), per_token.astype(BF16))
        slots = [
            jnp.sum(o * earlier, axis=1, keepdims=True).astype(jnp.int32) for o in onehot
        ]
        width = experts * PAIR
        place = lax.broadcasted_iota(jnp.int32, (rows, width), 1)
        pairs = [(o, p) for o, size in zip(outs, CHUNKS) for p in range(size // PAIR)]
        for i, (out_ref, p) in enumerate(pairs):
            weight = jnp.zeros((rows, width), F32)
            for k in range(top):
                local = slots[k] - i * PAIR
                inside = (local >= 0) & (local < PAIR)
                target = jnp.where(inside, ids[:, k : k + 1] * PAIR + local, -1)
                weight = jnp.where(target == place, gates[:, k : k + 1], weight)
            out_ref[:, p * width : (p + 1) * width] = weight.astype(BF16)

    return body


def matmul_halves(q_ref, xs, gate_ref, up_ref):
    n = gate_ref.shape[0]
    at = [lax.rem(q_ref[0] + s, n) for s in TURNS]
    gate = sum(dot(x, gate_ref[i]) for x, i in zip(xs, at))
    up = sum(dot(x, up_ref[i]) for x, i in zip(xs, at))
    return silu_times(gate, up)


def shared_body(q_ref, *refs):
    n = len(TURNS)
    gate_ref, up_ref, down_ref = refs[n : n + 3]
    outs = refs[n + 3 :]
    hidden = matmul_halves(q_ref, [r[...] for r in refs[:n]], gate_ref, up_ref)
    for s, out_ref in enumerate(outs):
        part = block(down_ref, lax.rem(q_ref[0] + s, n), out_ref.shape[1])
        out_ref[...] = dot(hidden, part).astype(BF16)


def ring_sums_body(q_ref, own_ref, left_ref, right_ref, gate_ref, up_ref, sums_ref, rest_ref):
    _, width, quarter = gate_ref.shape
    at = [lax.rem(q_ref[0] + s, len(TURNS)) for s in TURNS]
    half = own_ref.shape[0] // 2
    rows = sums_ref.shape[0] // 2
    for h in range(2):
        span = pl.ds(h * half, half)
        xs = [flat(r[span], width) for r in (own_ref, left_ref, right_ref)]
        out = pl.ds(h * rows, rows)
        sums_ref[out, :quarter] = sum(dot(x, gate_ref[i]) for x, i in zip(xs, at))
        sums_ref[out, quarter:] = sum(dot(x, up_ref[i]) for x, i in zip(xs, at))
    rest_ref[0] = gate_ref[at[3]]
    rest_ref[1] = up_ref[at[3]]


def ring_hidden_body(sums_ref, o0_ref, o1_ref, rest_ref, out_ref):
    _, width, quarter = rest_ref.shape
    x = jnp.concatenate([flat(o0_ref[...], width), flat(o1_ref[...], width)], axis=0)
    gate = sums_ref[:, :quarter] + dot(x, rest_ref[0])
    up = sums_ref[:, quarter:] + dot(x, rest_ref[1])
    out_ref[...] = silu_times(gate, up)


def pair_sums_body(q_ref, rows_ref, gate_ref, up_ref, sums_ref, rest_ref):
    _, width, quarter = gate_ref.shape
    at = [lax.rem(q_ref[0] + s, len(TURNS)) for s in TURNS]
    lanes = rows_ref.shape[2] // 2
    own = flat(rows_ref[:, :, :lanes], width)
    far = flat(rows_ref[:, :, lanes:], width)
    sums_ref[:, :quarter] = dot(own, gate_ref[at[0]]) + dot(far, gate_ref[at[3]])
    sums_ref[:, quarter:] = dot(own, up_ref[at[0]]) + dot(far, up_ref[at[3]])
    for i in range(2):
        rest_ref[2 * i] = gate_ref[at[1 + i]]
        rest_ref[2 * i + 1] = up_ref[at[1 + i]]


def pair_hidden_body(sums_ref, left_ref, right_ref, rest_ref, out_ref):
    _, width, quarter = rest_ref.shape
    left, right = flat(left_ref[...], width), flat(right_ref[...], width)
    gate = sums_ref[:, :quarter] + dot(left, rest_ref[0]) + dot(right, rest_ref[2])
    up = sums_ref[:, quarter:] + dot(left, rest_ref[1]) + dot(right, rest_ref[3])
    out_ref[...] = silu_times(gate, up)


def stack_body(*refs):
    *ins, out_ref = refs
    for s, ref in enumerate(ins):
        out_ref[s] = ref[...]


def down_body(halves):
    def body(*refs):
        *ins, down_ref, out_ref = refs
        count = out_ref.shape[0] // halves
        rows = ins[0].shape[0] // halves
        for h in range(halves):
            span = pl.ds(h * rows, rows)
            total = sum(dot(a[span], down_ref[s]) for s, a in enumerate(ins))
            unflat(out_ref.at[pl.ds(h * count, count)], total.astype(BF16))

    return body


def add_body(weight_ref, rows_ref, *refs):
    *parts, out_ref = refs
    rows = flat(rows_ref[...], out_ref.shape[1])
    total = sum((p[...].astype(F32) for p in parts), dot(weight_ref[...], rows))
    out_ref[...] = total.astype(out_ref.dtype)


def exchange(x, axis):
    return lax.all_to_all(x, axis, split_axis=0, concat_axis=0, tiled=True)


def shift(x, axis, by):
    n = lax.axis_size(axis)
    return lax.ppermute(x, axis, [(i, (i + by) % n) for i in range(n)])


def spread(x):
    return [x, shift(x, "tensor", 1), shift(x, "tensor", -1), shift(x, "tensor", 2)]


def deal(xs):
    return [xs[0], shift(xs[1], "tensor", 1), shift(xs[3], "tensor", -1), shift(xs[2], "tensor", 2)]


def ring(x):
    half = x.shape[0] // 2
    left = shift(x, "tensor", 1)
    right = shift(x, "tensor", -1)
    o0 = shift(left[:half], "tensor", 1)
    o1 = shift(right[half:], "tensor", -1)
    return left, right, o0, o1


def per_device(tokens, expert_ids, gate_values, w_gate, w_up, w_down, *shared):
    return layer(tokens, expert_ids, gate_values, w_gate, w_up, w_down[0], *shared)


def layer(
    tokens, expert_ids, gate_values, w_gate, w_up, w_down, shared_gate, shared_up, shared_down
):
    tok_dev, narrow = tokens.shape
    _, _, quarter = w_gate.shape
    experts = lax.axis_size(EXPERT)
    n = lax.axis_size("tensor")
    q = lax.axis_index("tensor").reshape(1)
    w_gate = w_gate.reshape(n, narrow, quarter)
    w_up = w_up.reshape(n, narrow, quarter)

    ids_t = expert_ids.T
    tokens_all = spread(tokens)
    ids_t = expert_ids.T
    arrived = []
    for j, (size, sources) in enumerate(zip(CHUNKS, ([tokens], [tokens, tokens_all[3]]))):
        (rows,) = kernel_call(
            gather_body(experts, sum(CHUNKS[:j]), size),
            [(experts, PAIR, len(sources) * size // PAIR * narrow)],
            ids_t,
            *sources,
        )
        arrived.append(exchange(rows, EXPERT))
    columns = kernel_call(columns_body, [(quarter, narrow)] * n, q, w_down, smem=1)
    (down,) = kernel_call(stack_body, [(n, quarter, narrow)], *deal(columns))
    weights = kernel_call(
        weight_body(experts),
        [(tok_dev, experts * size) for size in CHUNKS],
        expert_ids,
        gate_values,
    )
    shared_parts = kernel_call(
        shared_body,
        [(tok_dev, narrow)] * n,
        q,
        *tokens_all,
        shared_gate.reshape(n, narrow, -1),
        shared_up.reshape(n, narrow, -1),
        shared_down,
        smem=1,
        flops=10**9,
    )

    returned = []
    for j, (rows, size) in enumerate(zip(arrived, CHUNKS)):
        count = experts * size
        sums_shape = jax.ShapeDtypeStruct((count, 2 * quarter), F32)
        if j == 0:
            left, right, *last = ring(rows)
            args = (rows, left, right)
            bodies = ring_sums_body, ring_hidden_body
        else:
            own = rows[:, :, : size // PAIR * narrow]
            last = shift(own, "tensor", 1), shift(own, "tensor", -1)
            args = (rows,)
            bodies = pair_sums_body, pair_hidden_body
        sums, rest = kernel_call(
            bodies[0],
            [sums_shape, (2 * (1 + j), narrow, quarter)],
            q,
            *args,
            w_gate,
            w_up,
            smem=1,
            flops=10**9,
        )
        (hidden,) = kernel_call(bodies[1], [(count, quarter)], sums, *last, rest, flops=10**9)
        (out,) = kernel_call(
            down_body(2 - j),
            [(experts, PAIR, size // PAIR * narrow)],
            *spread(hidden),
            down,
            flops=10**9,
        )
        returned.append(exchange(out, EXPERT))
    shared_all = deal(shared_parts)
    total_shape = jax.ShapeDtypeStruct((tok_dev, narrow), F32)
    (total,) = kernel_call(add_body, [total_shape], weights[0], returned[0], *shared_all)
    return kernel_call(add_body, [(tok_dev, narrow)], weights[1], returned[1], total)[0]


def solution(mesh):
    torus = Mesh(
        mesh.devices.reshape(4, 8, 2, mesh.shape["tensor"]),
        ("expert_0", "expert_1", "expert_2", "tensor"),
    )
    placed = (
        P(EXPERT, "tensor"),
        P(EXPERT, None),
        P(EXPERT, None),
        P(EXPERT, None, "tensor"),
        P(EXPERT, None, "tensor"),
        P(EXPERT, "tensor", None),
        P(None, "tensor"),
        P(None, "tensor"),
        P("tensor", None),
    )
    return jax.shard_map(
        per_device, mesh=torus, in_specs=placed, out_specs=P(EXPERT, "tensor"), check_vma=False
    )
```

```python
import jax
import jax.numpy as jnp
from jax import lax
from jax.experimental import pallas as pl
from jax.experimental.pallas import tpu as pltpu
from jax.sharding import Mesh
from jax.sharding import PartitionSpec as P

EXPERT = ("expert_0", "expert_1", "expert_2")
CHUNKS = (6, 6)
PAIR = 2
TURNS = (0, 3, 1, 2)
F32 = jnp.float32
BF16 = jnp.bfloat16


def dot(a, b):
    return jnp.dot(a, b, preferred_element_type=F32)


def flat(x, width):
    count = x.shape[2] // width
    parts = [x[:, :, p * width : (p + 1) * width].reshape(-1, width) for p in range(count)]
    return jnp.concatenate(parts, axis=0)


def unflat(out_ref, x, lane=0):
    rows = out_ref.shape[0] * PAIR
    width = x.shape[1]
    for p in range(x.shape[0] // rows):
        part = x[p * rows : (p + 1) * rows].reshape(-1, PAIR, width)
        out_ref[:, :, lane + p * width : lane + (p + 1) * width] = part


def silu_times(gate, up):
    return (gate / (1.0 + jnp.exp(-gate)) * up).astype(BF16)


def kernel_call(body, outs, *args, smem=0, hbm=0, scratch=(), to_hbm=False, vmem=12, flops=1):
    places = [pltpu.SMEM] * smem + [pltpu.VMEM] * (len(args) - smem - hbm) + [pltpu.HBM] * hbm
    last = len(args) - hbm
    args = args[:last] + tuple(pltpu.with_memory_space_constraint(a, pltpu.HBM) for a in args[last:])
    return pl.pallas_call(
        body,
        in_specs=[pl.BlockSpec(memory_space=m) for m in places],
        out_specs=[pl.BlockSpec(memory_space=pltpu.HBM if to_hbm else pltpu.VMEM) for _ in outs],
        out_shape=[
            o
            if isinstance(o, jax.ShapeDtypeStruct)
            else (pltpu.HBM if to_hbm else jax.ShapeDtypeStruct)(o, BF16)
            for o in outs
        ],
        scratch_shapes=scratch,
        compiler_params=pltpu.CompilerParams(vmem_limit_bytes=vmem << 20),
        cost_estimate=pl.CostEstimate(flops=flops, transcendentals=0, bytes_accessed=0),
    )(*args)


def block(ref, index, width):
    return ref[:, pl.ds(pl.multiple_of(index * width, 128), width)]


def columns_body(q_ref, x_ref, *outs):
    n = len(outs)
    for s, out_ref in enumerate(outs):
        out_ref[...] = block(x_ref, lax.rem(q_ref[0] + s, n), out_ref.shape[1])


def gather_body(experts, first, size):
    def body(ids_ref, *refs):
        *tokens_refs, out_ref = refs
        ids = ids_ref[...]
        top, rows = ids.shape
        numbers = lax.broadcasted_iota(jnp.int32, (experts, rows), 0)
        onehot = [jnp.where(ids[k : k + 1] == numbers, 1.0, 0.0) for k in range(top)]
        per_token = sum(onehot[1:], onehot[0])
        before = lax.broadcasted_iota(jnp.int32, (rows, rows), 0) < lax.broadcasted_iota(
            jnp.int32, (rows, rows), 1
        )
        earlier = dot(per_token.astype(BF16), jnp.where(before, 1.0, 0.0).astype(BF16))
        slots = [
            jnp.sum(o * earlier, axis=0, keepdims=True).astype(jnp.int32) for o in onehot
        ]
        place = lax.broadcasted_iota(jnp.int32, (experts * PAIR, rows), 0)
        picks = []
        for p in range(first, first + size, PAIR):
            pick = jnp.zeros((experts * PAIR, rows), F32)
            for k in range(top):
                local = slots[k] - p
                inside = (local >= 0) & (local < PAIR)
                target = jnp.where(inside, ids[k : k + 1] * PAIR + local, -1)
                pick = jnp.where(target == place, 1.0, pick)
            picks.append(pick.astype(BF16))
        picks = jnp.concatenate(picks, axis=0)
        for s, tokens_ref in enumerate(tokens_refs):
            x = dot(picks, tokens_ref[...]).astype(BF16)
            unflat(out_ref, x, lane=s * (size // PAIR) * x.shape[1])

    return body


def weight_body(experts):
    def body(ids_ref, gates_ref, *outs):
        ids = ids_ref[...]
        gates = gates_ref[...].astype(F32)
        rows, top = ids.shape
        numbers = lax.broadcasted_iota(jnp.int32, (rows, experts), 1)
        onehot = [jnp.where(ids[:, k : k + 1] == numbers, 1.0, 0.0) for k in range(top)]
        per_token = sum(onehot[1:], onehot[0])
        before = lax.broadcasted_iota(jnp.int32, (rows, rows), 0) > lax.broadcasted_iota(
            jnp.int32, (rows, rows), 1
        )
        earlier = dot(jnp.where(before, 1.0, 0.0).astype(BF16), per_token.astype(BF16))
        slots = [
            jnp.sum(o * earlier, axis=1, keepdims=True).astype(jnp.int32) for o in onehot
        ]
        width = experts * PAIR
        place = lax.broadcasted_iota(jnp.int32, (rows, width), 1)
        pairs = [(o, p) for o, size in zip(outs, CHUNKS) for p in range(size // PAIR)]
        for i, (out_ref, p) in enumerate(pairs):
            weight = jnp.zeros((rows, width), F32)
            for k in range(top):
                local = slots[k] - i * PAIR
                inside = (local >= 0) & (local < PAIR)
                target = jnp.where(inside, ids[:, k : k + 1] * PAIR + local, -1)
                weight = jnp.where(target == place, gates[:, k : k + 1], weight)
            out_ref[:, p * width : (p + 1) * width] = weight.astype(BF16)

    return body


def matmul_halves(q_ref, xs, gate_ref, up_ref):
    n = gate_ref.shape[0]
    at = [lax.rem(q_ref[0] + s, n) for s in TURNS]
    gate = sum(dot(x, gate_ref[i]) for x, i in zip(xs, at))
    up = sum(dot(x, up_ref[i]) for x, i in zip(xs, at))
    return silu_times(gate, up)


def shared_body(q_ref, *refs):
    n = len(TURNS)
    gate_ref, up_ref, down_ref = refs[n : n + 3]
    outs = refs[n + 3 :]
    hidden = matmul_halves(q_ref, [r[...] for r in refs[:n]], gate_ref, up_ref)
    for s, out_ref in enumerate(outs):
        part = block(down_ref, lax.rem(q_ref[0] + s, n), out_ref.shape[1])
        out_ref[...] = dot(hidden, part).astype(BF16)


def ring_sums_body(q_ref, own_ref, left_ref, right_ref, gate_ref, up_ref, sums_ref, rest_ref):
    _, width, quarter = gate_ref.shape
    at = [lax.rem(q_ref[0] + s, len(TURNS)) for s in TURNS]
    half = own_ref.shape[0] // 2
    rows = sums_ref.shape[0] // 2
    for h in range(2):
        span = pl.ds(h * half, half)
        xs = [flat(r[span], width) for r in (own_ref, left_ref, right_ref)]
        out = pl.ds(h * rows, rows)
        sums_ref[out, :quarter] = sum(dot(x, gate_ref[i]) for x, i in zip(xs, at))
        sums_ref[out, quarter:] = sum(dot(x, up_ref[i]) for x, i in zip(xs, at))
    rest_ref[0] = gate_ref[at[3]]
    rest_ref[1] = up_ref[at[3]]


def ring_hidden_body(sums_ref, o0_ref, o1_ref, rest_ref, out_ref):
    _, width, quarter = rest_ref.shape
    x = jnp.concatenate([flat(o0_ref[...], width), flat(o1_ref[...], width)], axis=0)
    gate = sums_ref[:, :quarter] + dot(x, rest_ref[0])
    up = sums_ref[:, quarter:] + dot(x, rest_ref[1])
    out_ref[...] = silu_times(gate, up)


def pair_sums_body(q_ref, rows_ref, gate_hbm, up_hbm, sums_ref, *scratch):
    fetched = fetch(q_ref, (gate_hbm, up_hbm), (0, 3), *scratch)
    width, quarter = gate_hbm.shape[1:]
    lanes = rows_ref.shape[2] // 2
    xs = [flat(rows_ref[:, :, s * lanes : (s + 1) * lanes], width) for s in range(2)]
    sums_ref[...] = jnp.zeros_like(sums_ref)
    for x, pair in zip(xs, fetched):
        for k, take in enumerate(pair):
            sums_ref[:, k * quarter : (k + 1) * quarter] += dot(x, take())


def pair_hidden_body(q_ref, sums_ref, left_ref, right_ref, gate_hbm, up_hbm, out_ref, *scratch):
    fetched = fetch(q_ref, (gate_hbm, up_hbm), (1, 2), *scratch)
    width, quarter = gate_hbm.shape[1:]
    sums = [sums_ref[:, k * quarter : (k + 1) * quarter] for k in range(2)]
    for ref, pair in zip((left_ref, right_ref), fetched):
        x = flat(ref[...], width)
        sums = [total + dot(x, take()) for total, take in zip(sums, pair)]
    out_ref[...] = silu_times(*sums)


def fetch(q_ref, sources, turns, buffer, sems):
    def start(i, k, turn):
        at = lax.rem(q_ref[0] + TURNS[turn], sources[k].shape[0])
        copy = pltpu.make_async_copy(sources[k].at[at], buffer.at[i, k], sems.at[i, k])
        copy.start()

        def take():
            copy.wait()
            return buffer[i, k]

        return take

    return [[start(i, k, t) for k in range(len(sources))] for i, t in enumerate(turns)]


def down_body(halves):
    def body(*refs):
        n = len(TURNS)
        ins, parts, out_hbm = refs[:n], refs[n : 2 * n], refs[2 * n]
        rows_ref, down_ref, out_ref, in_sems, out_sems = refs[2 * n + 1 :]
        copies = []
        for s in range(n):
            pair = (
                pltpu.make_async_copy(ins[s], rows_ref.at[s], in_sems.at[0, s]),
                pltpu.make_async_copy(parts[s], down_ref.at[s], in_sems.at[1, s]),
            )
            for c in pair:
                c.start()
            copies.append(pair)
        total = 0.0
        for s in range(n):
            for c in copies[s]:
                c.wait()
            total = total + dot(rows_ref[s], down_ref[s])
        total = total.astype(BF16)
        count = out_ref.shape[0] // halves
        rows = total.shape[0] // halves
        leaving = []
        for h in range(halves):
            span = pl.ds(h * count, count)
            unflat(out_ref.at[span], total[h * rows : (h + 1) * rows])
            c = pltpu.make_async_copy(out_ref.at[span], out_hbm.at[span], out_sems.at[h])
            c.start()
            leaving.append(c)
        for c in leaving:
            c.wait()

    return body


def add_body(weight_ref, rows_ref, *refs):
    *parts, out_ref = refs
    rows = flat(rows_ref[...], out_ref.shape[1])
    total = sum((p[...].astype(F32) for p in parts), dot(weight_ref[...], rows))
    out_ref[...] = total.astype(out_ref.dtype)


def exchange(x, axis):
    return lax.all_to_all(x, axis, split_axis=0, concat_axis=0, tiled=True)


def shift(x, axis, by):
    n = lax.axis_size(axis)
    return lax.ppermute(x, axis, [(i, (i + by) % n) for i in range(n)])


def spread(x):
    return [x, shift(x, "tensor", 1), shift(x, "tensor", -1), shift(x, "tensor", 2)]


def deal(xs):
    return [xs[0], shift(xs[1], "tensor", 1), shift(xs[3], "tensor", -1), shift(xs[2], "tensor", 2)]


def ring(x):
    half = x.shape[0] // 2
    left = shift(x, "tensor", 1)
    right = shift(x, "tensor", -1)
    o0 = shift(left[:half], "tensor", 1)
    o1 = shift(right[half:], "tensor", -1)
    return left, right, o0, o1


def per_device(tokens, expert_ids, gate_values, w_gate, w_up, w_down, *shared):
    return layer(tokens, expert_ids, gate_values, w_gate, w_up, w_down[0], *shared)


def layer(
    tokens, expert_ids, gate_values, w_gate, w_up, w_down, shared_gate, shared_up, shared_down
):
    tok_dev, narrow = tokens.shape
    _, _, quarter = w_gate.shape
    experts = lax.axis_size(EXPERT)
    n = lax.axis_size("tensor")
    q = lax.axis_index("tensor").reshape(1)
    w_gate = w_gate.reshape(n, narrow, quarter)
    w_up = w_up.reshape(n, narrow, quarter)

    ids_t = expert_ids.T
    tokens_all = spread(tokens)
    ids_t = expert_ids.T
    arrived = []
    for j, (size, sources) in enumerate(zip(CHUNKS, ([tokens], [tokens, tokens_all[3]]))):
        (rows,) = kernel_call(
            gather_body(experts, sum(CHUNKS[:j]), size),
            [(experts, PAIR, len(sources) * size // PAIR * narrow)],
            ids_t,
            *sources,
        )
        arrived.append(exchange(rows, EXPERT))
    columns = kernel_call(columns_body, [(quarter, narrow)] * n, q, w_down, smem=1)
    down = deal(columns)
    weights = kernel_call(
        weight_body(experts),
        [(tok_dev, experts * size) for size in CHUNKS],
        expert_ids,
        gate_values,
    )
    shared_parts = kernel_call(
        shared_body,
        [(tok_dev, narrow)] * n,
        q,
        *tokens_all,
        shared_gate.reshape(n, narrow, -1),
        shared_up.reshape(n, narrow, -1),
        shared_down,
        smem=1,
        flops=10**9,
    )

    returned = []
    for j, (rows, size) in enumerate(zip(arrived, CHUNKS)):
        count = experts * size
        sums_shape = jax.ShapeDtypeStruct((count, 2 * quarter), F32)
        if j == 0:
            left, right, *last = ring(rows)
            args = (rows, left, right)
        else:
            own = rows[:, :, : size // PAIR * narrow]
            last = shift(own, "tensor", 1), shift(own, "tensor", -1)
            args = (rows,)
        if j == 0:
            sums, rest = kernel_call(
                ring_sums_body,
                [sums_shape, (2, narrow, quarter)],
                q,
                *args,
                w_gate,
                w_up,
                smem=1,
                flops=10**9,
            )
            (hidden,) = kernel_call(
                ring_hidden_body, [(count, quarter)], sums, *last, rest, flops=10**9
            )
        else:
            weights_hbm = dict(
                smem=1,
                hbm=2,
                scratch=[
                    pltpu.VMEM((2, 2, narrow, quarter), BF16),
                    pltpu.SemaphoreType.DMA((2, 2)),
                ],
                flops=10**9,
            )
            (sums,) = kernel_call(
                pair_sums_body, [sums_shape], q, *args, w_gate, w_up, **weights_hbm
            )
            (hidden,) = kernel_call(
                pair_hidden_body, [(count, quarter)], q, sums, *last, w_gate, w_up, **weights_hbm
            )
        out_shape = (experts, PAIR, size // PAIR * narrow)
        (out,) = kernel_call(
            down_body(2 - j),
            [out_shape],
            *spread(hidden),
            *down,
            hbm=2 * n,
            scratch=[
                pltpu.VMEM((n, count, quarter), BF16),
                pltpu.VMEM((n, quarter, narrow), BF16),
                pltpu.VMEM(out_shape, BF16),
                pltpu.SemaphoreType.DMA((2, n)),
                pltpu.SemaphoreType.DMA((2 - j,)),
            ],
            to_hbm=True,
            flops=10**9,
        )
        returned.append(exchange(out, EXPERT))
    shared_all = deal(shared_parts)
    total_shape = jax.ShapeDtypeStruct((tok_dev, narrow), F32)
    (total,) = kernel_call(add_body, [total_shape], weights[0], returned[0], *shared_all)
    return kernel_call(add_body, [(tok_dev, narrow)], weights[1], returned[1], total)[0]


def solution(mesh):
    torus = Mesh(
        mesh.devices.reshape(4, 8, 2, mesh.shape["tensor"]),
        ("expert_0", "expert_1", "expert_2", "tensor"),
    )
    placed = (
        P(EXPERT, "tensor"),
        P(EXPERT, None),
        P(EXPERT, None),
        P(EXPERT, None, "tensor"),
        P(EXPERT, None, "tensor"),
        P(EXPERT, "tensor", None),
        P(None, "tensor"),
        P(None, "tensor"),
        P("tensor", None),
    )
    return jax.shard_map(
        per_device, mesh=torus, in_specs=placed, out_specs=P(EXPERT, "tensor"), check_vma=False
    )
```

```python
import jax
import jax.numpy as jnp
from jax import lax
from jax.experimental import pallas as pl
from jax.experimental.pallas import tpu as pltpu
from jax.sharding import Mesh
from jax.sharding import PartitionSpec as P

EXPERT = ("expert_0", "expert_1", "expert_2")
CHUNKS = (6, 6)
PAIR = 2
TURNS = (0, 3, 1, 2)
F32 = jnp.float32
BF16 = jnp.bfloat16


def dot(a, b):
    return jnp.dot(a, b, preferred_element_type=F32)


def flat(x, width):
    count = x.shape[2] // width
    parts = [x[:, :, p * width : (p + 1) * width].reshape(-1, width) for p in range(count)]
    return jnp.concatenate(parts, axis=0)


def unflat(out_ref, x, lane=0):
    rows = out_ref.shape[0] * PAIR
    width = x.shape[1]
    for p in range(x.shape[0] // rows):
        part = x[p * rows : (p + 1) * rows].reshape(-1, PAIR, width)
        out_ref[:, :, lane + p * width : lane + (p + 1) * width] = part


def silu_times(gate, up):
    return (gate / (1.0 + jnp.exp(-gate)) * up).astype(BF16)


def kernel_call(body, outs, *args, smem=0, hbm=0, scratch=(), to_hbm=False, vmem=12, flops=1):
    places = [pltpu.SMEM] * smem + [pltpu.VMEM] * (len(args) - smem - hbm) + [pltpu.HBM] * hbm
    last = len(args) - hbm
    args = args[:last] + tuple(pltpu.with_memory_space_constraint(a, pltpu.HBM) for a in args[last:])
    return pl.pallas_call(
        body,
        in_specs=[pl.BlockSpec(memory_space=m) for m in places],
        out_specs=[pl.BlockSpec(memory_space=pltpu.HBM if to_hbm else pltpu.VMEM) for _ in outs],
        out_shape=[
            o
            if isinstance(o, jax.ShapeDtypeStruct)
            else (pltpu.HBM if to_hbm else jax.ShapeDtypeStruct)(o, BF16)
            for o in outs
        ],
        scratch_shapes=scratch,
        compiler_params=pltpu.CompilerParams(vmem_limit_bytes=vmem << 20),
        cost_estimate=pl.CostEstimate(flops=flops, transcendentals=0, bytes_accessed=0),
    )(*args)


def block(ref, index, width):
    return ref[:, pl.ds(pl.multiple_of(index * width, 128), width)]


def columns_body(q_ref, x_ref, *outs):
    n = len(outs)
    for s, out_ref in enumerate(outs):
        out_ref[...] = block(x_ref, lax.rem(q_ref[0] + s, n), out_ref.shape[1])


def gather_body(experts, first, size):
    def body(ids_ref, *refs):
        *tokens_refs, out_ref = refs
        ids = ids_ref[...]
        top, rows = ids.shape
        numbers = lax.broadcasted_iota(jnp.int32, (experts, rows), 0)
        onehot = [jnp.where(ids[k : k + 1] == numbers, 1.0, 0.0) for k in range(top)]
        per_token = sum(onehot[1:], onehot[0])
        before = lax.broadcasted_iota(jnp.int32, (rows, rows), 0) < lax.broadcasted_iota(
            jnp.int32, (rows, rows), 1
        )
        earlier = dot(per_token.astype(BF16), jnp.where(before, 1.0, 0.0).astype(BF16))
        slots = [
            jnp.sum(o * earlier, axis=0, keepdims=True).astype(jnp.int32) for o in onehot
        ]
        place = lax.broadcasted_iota(jnp.int32, (experts * PAIR, rows), 0)
        picks = []
        for p in range(first, first + size, PAIR):
            pick = jnp.zeros((experts * PAIR, rows), F32)
            for k in range(top):
                local = slots[k] - p
                inside = (local >= 0) & (local < PAIR)
                target = jnp.where(inside, ids[k : k + 1] * PAIR + local, -1)
                pick = jnp.where(target == place, 1.0, pick)
            picks.append(pick.astype(BF16))
        picks = jnp.concatenate(picks, axis=0)
        for s, tokens_ref in enumerate(tokens_refs):
            x = dot(picks, tokens_ref[...]).astype(BF16)
            unflat(out_ref, x, lane=s * (size // PAIR) * x.shape[1])

    return body


def weight_body(experts):
    def body(ids_ref, gates_ref, *outs):
        ids = ids_ref[...]
        gates = gates_ref[...].astype(F32)
        rows, top = ids.shape
        numbers = lax.broadcasted_iota(jnp.int32, (rows, experts), 1)
        onehot = [jnp.where(ids[:, k : k + 1] == numbers, 1.0, 0.0) for k in range(top)]
        per_token = sum(onehot[1:], onehot[0])
        before = lax.broadcasted_iota(jnp.int32, (rows, rows), 0) > lax.broadcasted_iota(
            jnp.int32, (rows, rows), 1
        )
        earlier = dot(jnp.where(before, 1.0, 0.0).astype(BF16), per_token.astype(BF16))
        slots = [
            jnp.sum(o * earlier, axis=1, keepdims=True).astype(jnp.int32) for o in onehot
        ]
        width = experts * PAIR
        place = lax.broadcasted_iota(jnp.int32, (rows, width), 1)
        pairs = [(o, p) for o, size in zip(outs, CHUNKS) for p in range(size // PAIR)]
        for i, (out_ref, p) in enumerate(pairs):
            weight = jnp.zeros((rows, width), F32)
            for k in range(top):
                local = slots[k] - i * PAIR
                inside = (local >= 0) & (local < PAIR)
                target = jnp.where(inside, ids[:, k : k + 1] * PAIR + local, -1)
                weight = jnp.where(target == place, gates[:, k : k + 1], weight)
            out_ref[:, p * width : (p + 1) * width] = weight.astype(BF16)

    return body


def matmul_halves(q_ref, xs, gate_ref, up_ref):
    n = gate_ref.shape[0]
    at = [lax.rem(q_ref[0] + s, n) for s in TURNS]
    gate = sum(dot(x, gate_ref[i]) for x, i in zip(xs, at))
    up = sum(dot(x, up_ref[i]) for x, i in zip(xs, at))
    return silu_times(gate, up)


def shared_body(q_ref, *refs):
    n = len(TURNS)
    gate_ref, up_ref, down_ref = refs[n : n + 3]
    outs = refs[n + 3 :]
    hidden = matmul_halves(q_ref, [r[...] for r in refs[:n]], gate_ref, up_ref)
    for s, out_ref in enumerate(outs):
        part = block(down_ref, lax.rem(q_ref[0] + s, n), out_ref.shape[1])
        out_ref[...] = dot(hidden, part).astype(BF16)


def ring_sums_body(q_ref, own_ref, left_ref, right_ref, gate_ref, up_ref, sums_ref, rest_ref):
    _, width, quarter = gate_ref.shape
    at = [lax.rem(q_ref[0] + s, len(TURNS)) for s in TURNS]
    half = own_ref.shape[0] // 2
    rows = sums_ref.shape[0] // 2
    for h in range(2):
        span = pl.ds(h * half, half)
        xs = [flat(r[span], width) for r in (own_ref, left_ref, right_ref)]
        out = pl.ds(h * rows, rows)
        sums_ref[out, :quarter] = sum(dot(x, gate_ref[i]) for x, i in zip(xs, at))
        sums_ref[out, quarter:] = sum(dot(x, up_ref[i]) for x, i in zip(xs, at))
    rest_ref[0] = gate_ref[at[3]]
    rest_ref[1] = up_ref[at[3]]


def ring_hidden_body(sums_ref, o0_ref, o1_ref, rest_ref, out_ref):
    _, width, quarter = rest_ref.shape
    x = jnp.concatenate([flat(o0_ref[...], width), flat(o1_ref[...], width)], axis=0)
    gate = sums_ref[:, :quarter] + dot(x, rest_ref[0])
    up = sums_ref[:, quarter:] + dot(x, rest_ref[1])
    out_ref[...] = silu_times(gate, up)


def pair_sums_body(q_ref, rows_ref, gate_ref, up_ref, sums_ref, rest_ref):
    _, width, quarter = gate_ref.shape
    at = [lax.rem(q_ref[0] + s, len(TURNS)) for s in TURNS]
    lanes = rows_ref.shape[2] // 2
    own = flat(rows_ref[:, :, :lanes], width)
    far = flat(rows_ref[:, :, lanes:], width)
    sums_ref[:, :quarter] = dot(own, gate_ref[at[0]]) + dot(far, gate_ref[at[3]])
    sums_ref[:, quarter:] = dot(own, up_ref[at[0]]) + dot(far, up_ref[at[3]])
    for i in range(2):
        rest_ref[2 * i] = gate_ref[at[1 + i]]
        rest_ref[2 * i + 1] = up_ref[at[1 + i]]


def pair_hidden_body(sums_ref, left_ref, right_ref, rest_ref, out_ref):
    _, width, quarter = rest_ref.shape
    left, right = flat(left_ref[...], width), flat(right_ref[...], width)
    gate = sums_ref[:, :quarter] + dot(left, rest_ref[0]) + dot(right, rest_ref[2])
    up = sums_ref[:, quarter:] + dot(left, rest_ref[1]) + dot(right, rest_ref[3])
    out_ref[...] = silu_times(gate, up)


def stack_body(*refs):
    *ins, out_ref = refs
    for s, ref in enumerate(ins):
        out_ref[s] = ref[...]


def down_body(halves):
    def body(*refs):
        n = len(TURNS)
        ins, parts, out_hbm = refs[:n], refs[n : 2 * n], refs[2 * n]
        rows_ref, down_ref, out_ref, in_sems, out_sems = refs[2 * n + 1 :]
        copies = []
        for s in range(n):
            pair = (
                pltpu.make_async_copy(ins[s], rows_ref.at[s], in_sems.at[0, s]),
                pltpu.make_async_copy(parts[s], down_ref.at[s], in_sems.at[1, s]),
            )
            for c in pair:
                c.start()
            copies.append(pair)
        total = 0.0
        for s in range(n):
            for c in copies[s]:
                c.wait()
            total = total + dot(rows_ref[s], down_ref[s])
        total = total.astype(BF16)
        count = out_ref.shape[0] // halves
        rows = total.shape[0] // halves
        leaving = []
        for h in range(halves):
            span = pl.ds(h * count, count)
            unflat(out_ref.at[span], total[h * rows : (h + 1) * rows])
            c = pltpu.make_async_copy(out_ref.at[span], out_hbm.at[span], out_sems.at[h])
            c.start()
            leaving.append(c)
        for c in leaving:
            c.wait()

    return body


def near_down_body(*refs):
    *ins, down_ref, out_ref = refs
    total = sum(dot(a[...], down_ref[s]) for s, a in enumerate(ins))
    unflat(out_ref, total.astype(BF16))


def halves_body(left_ref, right_ref, out0_ref, out1_ref):
    half = out0_ref.shape[0]
    out0_ref[...] = left_ref[pl.ds(0, half)]
    out1_ref[...] = right_ref[pl.ds(half, half)]


def own_body(rows_ref, out_ref):
    out_ref[...] = rows_ref[:, :, : out_ref.shape[2]]


def add_body(weight_ref, rows_ref, *refs):
    *parts, out_ref = refs
    rows = flat(rows_ref[...], out_ref.shape[1])
    total = sum((p[...].astype(F32) for p in parts), dot(weight_ref[...], rows))
    out_ref[...] = total.astype(out_ref.dtype)


def exchange(x, axis):
    return lax.all_to_all(x, axis, split_axis=0, concat_axis=0, tiled=True)


def shift(x, axis, by):
    n = lax.axis_size(axis)
    return lax.ppermute(x, axis, [(i, (i + by) % n) for i in range(n)])


def spread(x):
    return [x, shift(x, "tensor", 1), shift(x, "tensor", -1), shift(x, "tensor", 2)]


def deal(xs):
    return [xs[0], shift(xs[1], "tensor", 1), shift(xs[3], "tensor", -1), shift(xs[2], "tensor", 2)]


def ring(x):
    half = x.shape[0] // 2
    left = shift(x, "tensor", 1)
    right = shift(x, "tensor", -1)
    h0, h1 = kernel_call(halves_body, [(half, *x.shape[1:])] * 2, left, right)
    o0 = shift(h0, "tensor", 1)
    o1 = shift(h1, "tensor", -1)
    return left, right, o0, o1


def per_device(tokens, expert_ids, gate_values, w_gate, w_up, w_down, *shared):
    return layer(tokens, expert_ids, gate_values, w_gate, w_up, w_down[0], *shared)


def layer(
    tokens, expert_ids, gate_values, w_gate, w_up, w_down, shared_gate, shared_up, shared_down
):
    tok_dev, narrow = tokens.shape
    _, _, quarter = w_gate.shape
    experts = lax.axis_size(EXPERT)
    n = lax.axis_size("tensor")
    q = lax.axis_index("tensor").reshape(1)
    w_gate = w_gate.reshape(n, narrow, quarter)
    w_up = w_up.reshape(n, narrow, quarter)

    ids_t = expert_ids.T
    tokens_all = spread(tokens)
    ids_t = expert_ids.T
    arrived = []
    for j, (size, sources) in enumerate(zip(CHUNKS, ([tokens], [tokens, tokens_all[3]]))):
        (rows,) = kernel_call(
            gather_body(experts, sum(CHUNKS[:j]), size),
            [(experts, PAIR, len(sources) * size // PAIR * narrow)],
            ids_t,
            *sources,
        )
        arrived.append(exchange(rows, EXPERT))
    columns = kernel_call(columns_body, [(quarter, narrow)] * n, q, w_down, smem=1)
    down = deal(columns)
    weights = kernel_call(
        weight_body(experts),
        [(tok_dev, experts * size) for size in CHUNKS],
        expert_ids,
        gate_values,
    )
    shared_parts = kernel_call(
        shared_body,
        [(tok_dev, narrow)] * n,
        q,
        *tokens_all,
        shared_gate.reshape(n, narrow, -1),
        shared_up.reshape(n, narrow, -1),
        shared_down,
        smem=1,
        flops=10**9,
    )

    returned = []
    for j, (rows, size) in enumerate(zip(arrived, CHUNKS)):
        count = experts * size
        sums_shape = jax.ShapeDtypeStruct((count, 2 * quarter), F32)
        if j == 0:
            left, right, *last = ring(rows)
            args = (rows, left, right)
            bodies = ring_sums_body, ring_hidden_body
        else:
            own_shape = (experts, PAIR, size // PAIR * narrow)
            (own,) = kernel_call(own_body, [own_shape], rows)
            last = shift(own, "tensor", 1), shift(own, "tensor", -1)
            args = (rows,)
            bodies = pair_sums_body, pair_hidden_body
        sums, rest = kernel_call(
            bodies[0],
            [sums_shape, (2 * (1 + j), narrow, quarter)],
            q,
            *args,
            w_gate,
            w_up,
            smem=1,
            flops=10**9,
        )
        (hidden,) = kernel_call(bodies[1], [(count, quarter)], sums, *last, rest, flops=10**9)
        hidden_all = spread(hidden)
        out_shape = (experts, PAIR, size // PAIR * narrow)
        if j == 0:
            scratch = [
                pltpu.VMEM((n, count, quarter), BF16),
                pltpu.VMEM((n, quarter, narrow), BF16),
                pltpu.VMEM(out_shape, BF16),
                pltpu.SemaphoreType.DMA((2, n)),
                pltpu.SemaphoreType.DMA((2,)),
            ]
            (out,) = kernel_call(
                down_body(2),
                [out_shape],
                *hidden_all,
                *down,
                hbm=2 * n,
                scratch=scratch,
                to_hbm=True,
                flops=10**9,
            )
        else:
            (stacked,) = kernel_call(stack_body, [(n, quarter, narrow)], *down)
            (out,) = kernel_call(near_down_body, [out_shape], *hidden_all, stacked, flops=10**9)
        returned.append(exchange(out, EXPERT))
    shared_all = deal(shared_parts)
    total_shape = jax.ShapeDtypeStruct((tok_dev, narrow), F32)
    (total,) = kernel_call(add_body, [total_shape], weights[0], returned[0], *shared_all)
    return kernel_call(add_body, [(tok_dev, narrow)], weights[1], returned[1], total)[0]


def solution(mesh):
    torus = Mesh(
        mesh.devices.reshape(4, 8, 2, mesh.shape["tensor"]),
        ("expert_0", "expert_1", "expert_2", "tensor"),
    )
    placed = (
        P(EXPERT, "tensor"),
        P(EXPERT, None),
        P(EXPERT, None),
        P(EXPERT, None, "tensor"),
        P(EXPERT, None, "tensor"),
        P(EXPERT, "tensor", None),
        P(None, "tensor"),
        P(None, "tensor"),
        P("tensor", None),
    )
    return jax.shard_map(
        per_device, mesh=torus, in_specs=placed, out_specs=P(EXPERT, "tensor"), check_vma=False
    )
```

```python
import jax
import jax.numpy as jnp
from jax import lax
from jax.experimental import pallas as pl
from jax.experimental.pallas import tpu as pltpu
from jax.sharding import Mesh
from jax.sharding import PartitionSpec as P

EXPERT = ("expert_0", "expert_1", "expert_2")
CHUNKS = (6, 6)
PAIR = 2
TURNS = (0, 3, 1, 2)
F32 = jnp.float32
BF16 = jnp.bfloat16


def dot(a, b):
    return jnp.dot(a, b, preferred_element_type=F32)


def flat(x, width):
    count = x.shape[2] // width
    parts = [x[:, :, p * width : (p + 1) * width].reshape(-1, width) for p in range(count)]
    return jnp.concatenate(parts, axis=0)


def unflat(out_ref, x, lane=0):
    rows = out_ref.shape[0] * PAIR
    width = x.shape[1]
    for p in range(x.shape[0] // rows):
        part = x[p * rows : (p + 1) * rows].reshape(-1, PAIR, width)
        out_ref[:, :, lane + p * width : lane + (p + 1) * width] = part


def silu_times(gate, up):
    return (gate / (1.0 + jnp.exp(-gate)) * up).astype(BF16)


def kernel_call(body, outs, *args, smem=0, hbm=0, scratch=(), to_hbm=False, vmem=12, flops=1):
    places = [pltpu.SMEM] * smem + [pltpu.VMEM] * (len(args) - smem - hbm) + [pltpu.HBM] * hbm
    last = len(args) - hbm
    args = args[:last] + tuple(pltpu.with_memory_space_constraint(a, pltpu.HBM) for a in args[last:])
    return pl.pallas_call(
        body,
        in_specs=[pl.BlockSpec(memory_space=m) for m in places],
        out_specs=[pl.BlockSpec(memory_space=pltpu.HBM if to_hbm else pltpu.VMEM) for _ in outs],
        out_shape=[
            o
            if isinstance(o, jax.ShapeDtypeStruct)
            else (pltpu.HBM if to_hbm else jax.ShapeDtypeStruct)(o, BF16)
            for o in outs
        ],
        scratch_shapes=scratch,
        compiler_params=pltpu.CompilerParams(vmem_limit_bytes=vmem << 20),
        cost_estimate=pl.CostEstimate(flops=flops, transcendentals=0, bytes_accessed=0),
    )(*args)


def block(ref, index, width):
    return ref[:, pl.ds(pl.multiple_of(index * width, 128), width)]


def columns_body(q_ref, x_ref, *outs):
    n = len(outs)
    for s, out_ref in enumerate(outs):
        out_ref[...] = block(x_ref, lax.rem(q_ref[0] + s, n), out_ref.shape[1])


def gather_body(experts, first, size):
    def fetching(ids_hbm, tokens_hbm, out_ref, ids_ref, tokens_ref, sems):
        pairs = ((ids_hbm, ids_ref), (tokens_hbm, tokens_ref))
        copies = [pltpu.make_async_copy(a, b, sems.at[i]) for i, (a, b) in enumerate(pairs)]
        for c in copies:
            c.start()
        copies[0].wait()
        picks = choose(ids_ref[...])
        copies[1].wait()
        unflat(out_ref, dot(picks, tokens_ref[...]).astype(BF16))

    def body(ids_ref, *refs):
        *tokens_refs, out_ref = refs
        picks = choose(ids_ref[...])
        for s, tokens_ref in enumerate(tokens_refs):
            x = dot(picks, tokens_ref[...]).astype(BF16)
            unflat(out_ref, x, lane=s * (size // PAIR) * x.shape[1])

    def choose(ids):
        top, rows = ids.shape
        numbers = lax.broadcasted_iota(jnp.int32, (experts, rows), 0)
        onehot = [jnp.where(ids[k : k + 1] == numbers, 1.0, 0.0) for k in range(top)]
        per_token = sum(onehot[1:], onehot[0])
        before = lax.broadcasted_iota(jnp.int32, (rows, rows), 0) < lax.broadcasted_iota(
            jnp.int32, (rows, rows), 1
        )
        earlier = dot(per_token.astype(BF16), jnp.where(before, 1.0, 0.0).astype(BF16))
        slots = [
            jnp.sum(o * earlier, axis=0, keepdims=True).astype(jnp.int32) for o in onehot
        ]
        place = lax.broadcasted_iota(jnp.int32, (experts * PAIR, rows), 0)
        picks = []
        for p in range(first, first + size, PAIR):
            pick = jnp.zeros((experts * PAIR, rows), F32)
            for k in range(top):
                local = slots[k] - p
                inside = (local >= 0) & (local < PAIR)
                target = jnp.where(inside, ids[k : k + 1] * PAIR + local, -1)
                pick = jnp.where(target == place, 1.0, pick)
            picks.append(pick.astype(BF16))
        return jnp.concatenate(picks, axis=0)

    return body if first else fetching


def weight_body(experts):
    def body(ids_ref, gates_ref, *outs):
        ids = ids_ref[...]
        gates = gates_ref[...].astype(F32)
        rows, top = ids.shape
        numbers = lax.broadcasted_iota(jnp.int32, (rows, experts), 1)
        onehot = [jnp.where(ids[:, k : k + 1] == numbers, 1.0, 0.0) for k in range(top)]
        per_token = sum(onehot[1:], onehot[0])
        before = lax.broadcasted_iota(jnp.int32, (rows, rows), 0) > lax.broadcasted_iota(
            jnp.int32, (rows, rows), 1
        )
        earlier = dot(jnp.where(before, 1.0, 0.0).astype(BF16), per_token.astype(BF16))
        slots = [
            jnp.sum(o * earlier, axis=1, keepdims=True).astype(jnp.int32) for o in onehot
        ]
        width = experts * PAIR
        place = lax.broadcasted_iota(jnp.int32, (rows, width), 1)
        pairs = [(o, p) for o, size in zip(outs, CHUNKS) for p in range(size // PAIR)]
        for i, (out_ref, p) in enumerate(pairs):
            weight = jnp.zeros((rows, width), F32)
            for k in range(top):
                local = slots[k] - i * PAIR
                inside = (local >= 0) & (local < PAIR)
                target = jnp.where(inside, ids[:, k : k + 1] * PAIR + local, -1)
                weight = jnp.where(target == place, gates[:, k : k + 1], weight)
            out_ref[:, p * width : (p + 1) * width] = weight.astype(BF16)

    return body


def matmul_halves(q_ref, xs, gate_ref, up_ref):
    n = gate_ref.shape[0]
    at = [lax.rem(q_ref[0] + s, n) for s in TURNS]
    gate = sum(dot(x, gate_ref[i]) for x, i in zip(xs, at))
    up = sum(dot(x, up_ref[i]) for x, i in zip(xs, at))
    return silu_times(gate, up)


def shared_body(q_ref, *refs):
    n = len(TURNS)
    gate_ref, up_ref, down_ref = refs[n : n + 3]
    outs = refs[n + 3 :]
    hidden = matmul_halves(q_ref, [r[...] for r in refs[:n]], gate_ref, up_ref)
    for s, out_ref in enumerate(outs):
        part = block(down_ref, lax.rem(q_ref[0] + s, n), out_ref.shape[1])
        out_ref[...] = dot(hidden, part).astype(BF16)


def ring_sums_body(q_ref, own_ref, left_ref, right_ref, gate_ref, up_ref, sums_ref, rest_ref):
    _, width, quarter = gate_ref.shape
    at = [lax.rem(q_ref[0] + s, len(TURNS)) for s in TURNS]
    half = own_ref.shape[0] // 2
    rows = sums_ref.shape[0] // 2
    for h in range(2):
        span = pl.ds(h * half, half)
        xs = [flat(r[span], width) for r in (own_ref, left_ref, right_ref)]
        out = pl.ds(h * rows, rows)
        sums_ref[out, :quarter] = sum(dot(x, gate_ref[i]) for x, i in zip(xs, at))
        sums_ref[out, quarter:] = sum(dot(x, up_ref[i]) for x, i in zip(xs, at))
    rest_ref[0] = gate_ref[at[3]]
    rest_ref[1] = up_ref[at[3]]


def ring_hidden_body(sums_ref, o0_ref, o1_ref, rest_ref, out_ref):
    _, width, quarter = rest_ref.shape
    x = jnp.concatenate([flat(o0_ref[...], width), flat(o1_ref[...], width)], axis=0)
    gate = sums_ref[:, :quarter] + dot(x, rest_ref[0])
    up = sums_ref[:, quarter:] + dot(x, rest_ref[1])
    out_ref[...] = silu_times(gate, up)


def pair_sums_body(q_ref, rows_ref, gate_ref, up_ref, sums_ref, rest_ref):
    _, width, quarter = gate_ref.shape
    at = [lax.rem(q_ref[0] + s, len(TURNS)) for s in TURNS]
    lanes = rows_ref.shape[2] // 2
    own = flat(rows_ref[:, :, :lanes], width)
    far = flat(rows_ref[:, :, lanes:], width)
    sums_ref[:, :quarter] = dot(own, gate_ref[at[0]]) + dot(far, gate_ref[at[3]])
    sums_ref[:, quarter:] = dot(own, up_ref[at[0]]) + dot(far, up_ref[at[3]])
    for i in range(2):
        rest_ref[2 * i] = gate_ref[at[1 + i]]
        rest_ref[2 * i + 1] = up_ref[at[1 + i]]


def pair_hidden_body(sums_ref, left_ref, right_ref, rest_ref, out_ref):
    _, width, quarter = rest_ref.shape
    left, right = flat(left_ref[...], width), flat(right_ref[...], width)
    gate = sums_ref[:, :quarter] + dot(left, rest_ref[0]) + dot(right, rest_ref[2])
    up = sums_ref[:, quarter:] + dot(left, rest_ref[1]) + dot(right, rest_ref[3])
    out_ref[...] = silu_times(gate, up)


def stack_body(*refs):
    *ins, out_ref = refs
    for s, ref in enumerate(ins):
        out_ref[s] = ref[...]


def down_body(halves):
    def body(*refs):
        n = len(TURNS)
        ins, parts, out_hbm = refs[:n], refs[n : 2 * n], refs[2 * n]
        rows_ref, down_ref, out_ref, in_sems, out_sems = refs[2 * n + 1 :]
        copies = []
        for s in range(n):
            pair = (
                pltpu.make_async_copy(ins[s], rows_ref.at[s], in_sems.at[0, s]),
                pltpu.make_async_copy(parts[s], down_ref.at[s], in_sems.at[1, s]),
            )
            for c in pair:
                c.start()
            copies.append(pair)
        total = 0.0
        for s in range(n):
            for c in copies[s]:
                c.wait()
            total = total + dot(rows_ref[s], down_ref[s])
        total = total.astype(BF16)
        count = out_ref.shape[0] // halves
        rows = total.shape[0] // halves
        leaving = []
        for h in range(halves):
            span = pl.ds(h * count, count)
            unflat(out_ref.at[span], total[h * rows : (h + 1) * rows])
            c = pltpu.make_async_copy(out_ref.at[span], out_hbm.at[span], out_sems.at[h])
            c.start()
            leaving.append(c)
        for c in leaving:
            c.wait()

    return body


def near_down_body(*refs):
    *ins, down_ref, out_ref = refs
    total = sum(dot(a[...], down_ref[s]) for s, a in enumerate(ins))
    unflat(out_ref, total.astype(BF16))


def halves_body(left_ref, right_ref, out0_ref, out1_ref):
    half = out0_ref.shape[0]
    out0_ref[...] = left_ref[pl.ds(0, half)]
    out1_ref[...] = right_ref[pl.ds(half, half)]


def own_body(rows_ref, out_ref):
    out_ref[...] = rows_ref[:, :, : out_ref.shape[2]]


def add_body(weight_ref, rows_ref, *refs):
    *parts, out_ref = refs
    rows = flat(rows_ref[...], out_ref.shape[1])
    total = sum((p[...].astype(F32) for p in parts), dot(weight_ref[...], rows))
    out_ref[...] = total.astype(out_ref.dtype)


def exchange(x, axis):
    return lax.all_to_all(x, axis, split_axis=0, concat_axis=0, tiled=True)


def shift(x, axis, by):
    n = lax.axis_size(axis)
    return lax.ppermute(x, axis, [(i, (i + by) % n) for i in range(n)])


def spread(x):
    return [x, shift(x, "tensor", 1), shift(x, "tensor", -1), shift(x, "tensor", 2)]


def deal(xs):
    return [xs[0], shift(xs[1], "tensor", 1), shift(xs[3], "tensor", -1), shift(xs[2], "tensor", 2)]


def ring(x):
    half = x.shape[0] // 2
    left = shift(x, "tensor", 1)
    right = shift(x, "tensor", -1)
    h0, h1 = kernel_call(halves_body, [(half, *x.shape[1:])] * 2, left, right)
    o0 = shift(h0, "tensor", 1)
    o1 = shift(h1, "tensor", -1)
    return left, right, o0, o1


def per_device(tokens, expert_ids, gate_values, w_gate, w_up, w_down, *shared):
    return layer(tokens, expert_ids, gate_values, w_gate, w_up, w_down[0], *shared)


def layer(
    tokens, expert_ids, gate_values, w_gate, w_up, w_down, shared_gate, shared_up, shared_down
):
    tok_dev, narrow = tokens.shape
    _, _, quarter = w_gate.shape
    experts = lax.axis_size(EXPERT)
    n = lax.axis_size("tensor")
    q = lax.axis_index("tensor").reshape(1)
    w_gate = w_gate.reshape(n, narrow, quarter)
    w_up = w_up.reshape(n, narrow, quarter)

    ids_t = expert_ids.T
    tokens_all = spread(tokens)
    ids_t = expert_ids.T
    arrived = []
    for j, (size, sources) in enumerate(zip(CHUNKS, ([tokens], [tokens, tokens_all[3]]))):
        scratch = [
            pltpu.VMEM(ids_t.shape, jnp.int32),
            pltpu.VMEM(tokens.shape, BF16),
            pltpu.SemaphoreType.DMA((2,)),
        ]
        (rows,) = kernel_call(
            gather_body(experts, sum(CHUNKS[:j]), size),
            [(experts, PAIR, len(sources) * size // PAIR * narrow)],
            ids_t,
            *sources,
            **({} if j else dict(hbm=2, scratch=scratch)),
        )
        arrived.append(exchange(rows, EXPERT))
    columns = kernel_call(columns_body, [(quarter, narrow)] * n, q, w_down, smem=1)
    down = deal(columns)
    weights = kernel_call(
        weight_body(experts),
        [(tok_dev, experts * size) for size in CHUNKS],
        expert_ids,
        gate_values,
    )
    shared_parts = kernel_call(
        shared_body,
        [(tok_dev, narrow)] * n,
        q,
        *tokens_all,
        shared_gate.reshape(n, narrow, -1),
        shared_up.reshape(n, narrow, -1),
        shared_down,
        smem=1,
        flops=10**9,
    )

    returned = []
    for j, (rows, size) in enumerate(zip(arrived, CHUNKS)):
        count = experts * size
        sums_shape = jax.ShapeDtypeStruct((count, 2 * quarter), F32)
        if j == 0:
            left, right, *last = ring(rows)
            args = (rows, left, right)
            bodies = ring_sums_body, ring_hidden_body
        else:
            own_shape = (experts, PAIR, size // PAIR * narrow)
            (own,) = kernel_call(own_body, [own_shape], rows)
            last = shift(own, "tensor", 1), shift(own, "tensor", -1)
            args = (rows,)
            bodies = pair_sums_body, pair_hidden_body
        sums, rest = kernel_call(
            bodies[0],
            [sums_shape, (2 * (1 + j), narrow, quarter)],
            q,
            *args,
            w_gate,
            w_up,
            smem=1,
            flops=10**9,
        )
        (hidden,) = kernel_call(bodies[1], [(count, quarter)], sums, *last, rest, flops=10**9)
        hidden_all = spread(hidden)
        out_shape = (experts, PAIR, size // PAIR * narrow)
        if j == 0:
            scratch = [
                pltpu.VMEM((n, count, quarter), BF16),
                pltpu.VMEM((n, quarter, narrow), BF16),
                pltpu.VMEM(out_shape, BF16),
                pltpu.SemaphoreType.DMA((2, n)),
                pltpu.SemaphoreType.DMA((2,)),
            ]
            (out,) = kernel_call(
                down_body(2),
                [out_shape],
                *hidden_all,
                *down,
                hbm=2 * n,
                scratch=scratch,
                to_hbm=True,
                flops=10**9,
            )
        else:
            (stacked,) = kernel_call(stack_body, [(n, quarter, narrow)], *down)
            (out,) = kernel_call(near_down_body, [out_shape], *hidden_all, stacked, flops=10**9)
        returned.append(exchange(out, EXPERT))
    shared_all = deal(shared_parts)
    total_shape = jax.ShapeDtypeStruct((tok_dev, narrow), F32)
    (total,) = kernel_call(add_body, [total_shape], weights[0], returned[0], *shared_all)
    return kernel_call(add_body, [(tok_dev, narrow)], weights[1], returned[1], total)[0]


def solution(mesh):
    torus = Mesh(
        mesh.devices.reshape(4, 8, 2, mesh.shape["tensor"]),
        ("expert_0", "expert_1", "expert_2", "tensor"),
    )
    placed = (
        P(EXPERT, "tensor"),
        P(EXPERT, None),
        P(EXPERT, None),
        P(EXPERT, None, "tensor"),
        P(EXPERT, None, "tensor"),
        P(EXPERT, "tensor", None),
        P(None, "tensor"),
        P(None, "tensor"),
        P("tensor", None),
    )
    return jax.shard_map(
        per_device, mesh=torus, in_specs=placed, out_specs=P(EXPERT, "tensor"), check_vma=False
    )
```

```python
import jax
import jax.numpy as jnp
from jax import lax
from jax.experimental import pallas as pl
from jax.experimental.pallas import tpu as pltpu
from jax.sharding import Mesh
from jax.sharding import PartitionSpec as P

EXPERT = ("expert_0", "expert_1", "expert_2")
CHUNKS = (6, 6)
PAIR = 2
TURNS = (0, 3, 1, 2)
F32 = jnp.float32
BF16 = jnp.bfloat16


def dot(a, b):
    return jnp.dot(a, b, preferred_element_type=F32)


def flat(x, width):
    count = x.shape[2] // width
    parts = [x[:, :, p * width : (p + 1) * width].reshape(-1, width) for p in range(count)]
    return jnp.concatenate(parts, axis=0)


def unflat(out_ref, x, lane=0):
    rows = out_ref.shape[0] * PAIR
    width = x.shape[1]
    for p in range(x.shape[0] // rows):
        part = x[p * rows : (p + 1) * rows].reshape(-1, PAIR, width)
        out_ref[:, :, lane + p * width : lane + (p + 1) * width] = part


def silu_times(gate, up):
    return (gate / (1.0 + jnp.exp(-gate)) * up).astype(BF16)


def kernel_call(body, outs, *args, smem=0, hbm=0, scratch=(), to_hbm=False, vmem=12, flops=1):
    places = [pltpu.SMEM] * smem + [pltpu.VMEM] * (len(args) - smem - hbm) + [pltpu.HBM] * hbm
    last = len(args) - hbm
    args = args[:last] + tuple(pltpu.with_memory_space_constraint(a, pltpu.HBM) for a in args[last:])
    return pl.pallas_call(
        body,
        in_specs=[pl.BlockSpec(memory_space=m) for m in places],
        out_specs=[pl.BlockSpec(memory_space=pltpu.HBM if to_hbm else pltpu.VMEM) for _ in outs],
        out_shape=[
            o
            if isinstance(o, jax.ShapeDtypeStruct)
            else (pltpu.HBM if to_hbm else jax.ShapeDtypeStruct)(o, BF16)
            for o in outs
        ],
        scratch_shapes=scratch,
        compiler_params=pltpu.CompilerParams(vmem_limit_bytes=vmem << 20),
        cost_estimate=pl.CostEstimate(flops=flops, transcendentals=0, bytes_accessed=0),
    )(*args)


def block(ref, index, width):
    return ref[:, pl.ds(pl.multiple_of(index * width, 128), width)]


def columns_body(q_ref, x_ref, *outs):
    n = len(outs)
    for s, out_ref in enumerate(outs):
        out_ref[...] = block(x_ref, lax.rem(q_ref[0] + s, n), out_ref.shape[1])


def gather_body(experts, first, size):
    def fetching(ids_hbm, tokens_hbm, out_ref, ids_ref, tokens_ref, sems):
        pairs = ((ids_hbm, ids_ref), (tokens_hbm, tokens_ref))
        copies = [pltpu.make_async_copy(a, b, sems.at[i]) for i, (a, b) in enumerate(pairs)]
        for c in copies:
            c.start()
        copies[0].wait()
        picks = choose(ids_ref[...])
        copies[1].wait()
        unflat(out_ref, dot(picks, tokens_ref[...]).astype(BF16))

    def body(ids_ref, *refs):
        *tokens_refs, out_ref = refs
        picks = choose(ids_ref[...])
        for s, tokens_ref in enumerate(tokens_refs):
            x = dot(picks, tokens_ref[...]).astype(BF16)
            unflat(out_ref, x, lane=s * (size // PAIR) * x.shape[1])

    def choose(ids):
        top, rows = ids.shape
        numbers = lax.broadcasted_iota(jnp.int32, (experts, rows), 0)
        onehot = [jnp.where(ids[k : k + 1] == numbers, 1.0, 0.0) for k in range(top)]
        per_token = sum(onehot[1:], onehot[0])
        before = lax.broadcasted_iota(jnp.int32, (rows, rows), 0) < lax.broadcasted_iota(
            jnp.int32, (rows, rows), 1
        )
        earlier = dot(per_token.astype(BF16), jnp.where(before, 1.0, 0.0).astype(BF16))
        slots = [
            jnp.sum(o * earlier, axis=0, keepdims=True).astype(jnp.int32) for o in onehot
        ]
        place = lax.broadcasted_iota(jnp.int32, (experts * PAIR, rows), 0)
        picks = []
        for p in range(first, first + size, PAIR):
            pick = jnp.zeros((experts * PAIR, rows), F32)
            for k in range(top):
                local = slots[k] - p
                inside = (local >= 0) & (local < PAIR)
                target = jnp.where(inside, ids[k : k + 1] * PAIR + local, -1)
                pick = jnp.where(target == place, 1.0, pick)
            picks.append(pick.astype(BF16))
        return jnp.concatenate(picks, axis=0)

    return body if first else fetching


def weight_body(experts):
    def body(ids_ref, gates_ref, *outs):
        ids = ids_ref[...]
        gates = gates_ref[...].astype(F32)
        rows, top = ids.shape
        numbers = lax.broadcasted_iota(jnp.int32, (rows, experts), 1)
        onehot = [jnp.where(ids[:, k : k + 1] == numbers, 1.0, 0.0) for k in range(top)]
        per_token = sum(onehot[1:], onehot[0])
        before = lax.broadcasted_iota(jnp.int32, (rows, rows), 0) > lax.broadcasted_iota(
            jnp.int32, (rows, rows), 1
        )
        earlier = dot(jnp.where(before, 1.0, 0.0).astype(BF16), per_token.astype(BF16))
        slots = [
            jnp.sum(o * earlier, axis=1, keepdims=True).astype(jnp.int32) for o in onehot
        ]
        width = experts * PAIR
        place = lax.broadcasted_iota(jnp.int32, (rows, width), 1)
        pairs = [(o, p) for o, size in zip(outs, CHUNKS) for p in range(size // PAIR)]
        for i, (out_ref, p) in enumerate(pairs):
            weight = jnp.zeros((rows, width), F32)
            for k in range(top):
                local = slots[k] - i * PAIR
                inside = (local >= 0) & (local < PAIR)
                target = jnp.where(inside, ids[:, k : k + 1] * PAIR + local, -1)
                weight = jnp.where(target == place, gates[:, k : k + 1], weight)
            out_ref[:, p * width : (p + 1) * width] = weight.astype(BF16)

    return body


def matmul_halves(q_ref, xs, gate_ref, up_ref):
    n = gate_ref.shape[0]
    at = [lax.rem(q_ref[0] + s, n) for s in TURNS]
    gate = sum(dot(x, gate_ref[i]) for x, i in zip(xs, at))
    up = sum(dot(x, up_ref[i]) for x, i in zip(xs, at))
    return silu_times(gate, up)


def shared_body(q_ref, *refs):
    n = len(TURNS)
    gate_ref, up_ref, down_ref = refs[n : n + 3]
    outs = refs[n + 3 :]
    hidden = matmul_halves(q_ref, [r[...] for r in refs[:n]], gate_ref, up_ref)
    for s, out_ref in enumerate(outs):
        part = block(down_ref, lax.rem(q_ref[0] + s, n), out_ref.shape[1])
        out_ref[...] = dot(hidden, part).astype(BF16)


def ring_sums_body(q_ref, own_ref, left_ref, right_ref, gate_ref, up_ref, sums_ref, rest_ref):
    _, width, quarter = gate_ref.shape
    at = [lax.rem(q_ref[0] + s, len(TURNS)) for s in TURNS]
    half = own_ref.shape[0] // 2
    rows = sums_ref.shape[0] // 2
    for h in range(2):
        span = pl.ds(h * half, half)
        xs = [flat(r[span], width) for r in (own_ref, left_ref, right_ref)]
        out = pl.ds(h * rows, rows)
        sums_ref[out, :quarter] = sum(dot(x, gate_ref[i]) for x, i in zip(xs, at))
        sums_ref[out, quarter:] = sum(dot(x, up_ref[i]) for x, i in zip(xs, at))
    rest_ref[0] = gate_ref[at[3]]
    rest_ref[1] = up_ref[at[3]]


def ring_hidden_body(sums_ref, o0_ref, o1_ref, rest_ref, out_ref):
    _, width, quarter = rest_ref.shape
    x = jnp.concatenate([flat(o0_ref[...], width), flat(o1_ref[...], width)], axis=0)
    gate = sums_ref[:, :quarter] + dot(x, rest_ref[0])
    up = sums_ref[:, quarter:] + dot(x, rest_ref[1])
    out_ref[...] = silu_times(gate, up)


def pair_sums_body(q_ref, rows_ref, gate_ref, up_ref, sums_ref, rest_ref):
    _, width, quarter = gate_ref.shape
    at = [lax.rem(q_ref[0] + s, len(TURNS)) for s in TURNS]
    lanes = rows_ref.shape[2] // 2
    own = flat(rows_ref[:, :, :lanes], width)
    far = flat(rows_ref[:, :, lanes:], width)
    sums_ref[:, :quarter] = dot(own, gate_ref[at[0]]) + dot(far, gate_ref[at[3]])
    sums_ref[:, quarter:] = dot(own, up_ref[at[0]]) + dot(far, up_ref[at[3]])
    for i in range(2):
        rest_ref[2 * i] = gate_ref[at[1 + i]]
        rest_ref[2 * i + 1] = up_ref[at[1 + i]]


def pair_hidden_body(sums_ref, left_ref, right_ref, rest_ref, out_ref):
    _, width, quarter = rest_ref.shape
    left, right = flat(left_ref[...], width), flat(right_ref[...], width)
    gate = sums_ref[:, :quarter] + dot(left, rest_ref[0]) + dot(right, rest_ref[2])
    up = sums_ref[:, quarter:] + dot(left, rest_ref[1]) + dot(right, rest_ref[3])
    out_ref[...] = silu_times(gate, up)


def stack_body(*refs):
    *ins, out_ref = refs
    for s, ref in enumerate(ins):
        out_ref[s] = ref[...]


def stack_copies_body(*refs):
    *ins, out_ref, sems = refs
    copies = [pltpu.make_async_copy(a, out_ref.at[s], sems.at[s]) for s, a in enumerate(ins)]
    for c in copies:
        c.start()
    for c in copies:
        c.wait()


def down_body(halves):
    def body(down_ref, *refs):
        n = len(TURNS)
        ins, out_hbm = refs[:n], refs[n]
        rows_ref, out_ref, in_sems, out_sems = refs[n + 1 :]
        copies = [
            pltpu.make_async_copy(ins[s], rows_ref.at[s], in_sems.at[s]) for s in range(n)
        ]
        for c in copies:
            c.start()
        total = 0.0
        for s in range(n):
            copies[s].wait()
            total = total + dot(rows_ref[s], down_ref[s])
        total = total.astype(BF16)
        count = out_ref.shape[0] // halves
        rows = total.shape[0] // halves
        leaving = []
        for h in range(halves):
            span = pl.ds(h * count, count)
            unflat(out_ref.at[span], total[h * rows : (h + 1) * rows])
            c = pltpu.make_async_copy(out_ref.at[span], out_hbm.at[span], out_sems.at[h])
            c.start()
            leaving.append(c)
        for c in leaving:
            c.wait()

    return body


def near_down_body(*refs):
    *ins, down_ref, out_ref = refs
    total = sum(dot(a[...], down_ref[s]) for s, a in enumerate(ins))
    unflat(out_ref, total.astype(BF16))


def halves_body(left_ref, right_ref, out0_ref, out1_ref):
    half = out0_ref.shape[0]
    out0_ref[...] = left_ref[pl.ds(0, half)]
    out1_ref[...] = right_ref[pl.ds(half, half)]


def own_body(rows_ref, out_ref):
    out_ref[...] = rows_ref[:, :, : out_ref.shape[2]]


def add_body(weight_ref, rows_ref, *refs):
    *parts, out_ref = refs
    rows = flat(rows_ref[...], out_ref.shape[1])
    total = sum((p[...].astype(F32) for p in parts), dot(weight_ref[...], rows))
    out_ref[...] = total.astype(out_ref.dtype)


def exchange(x, axis):
    return lax.all_to_all(x, axis, split_axis=0, concat_axis=0, tiled=True)


def shift(x, axis, by):
    n = lax.axis_size(axis)
    return lax.ppermute(x, axis, [(i, (i + by) % n) for i in range(n)])


def spread(x):
    return [x, shift(x, "tensor", 1), shift(x, "tensor", -1), shift(x, "tensor", 2)]


def deal(xs):
    return [xs[0], shift(xs[1], "tensor", 1), shift(xs[3], "tensor", -1), shift(xs[2], "tensor", 2)]


def ring(x):
    half = x.shape[0] // 2
    left = shift(x, "tensor", 1)
    right = shift(x, "tensor", -1)
    h0, h1 = kernel_call(halves_body, [(half, *x.shape[1:])] * 2, left, right)
    o0 = shift(h0, "tensor", 1)
    o1 = shift(h1, "tensor", -1)
    return left, right, o0, o1


def per_device(tokens, expert_ids, gate_values, w_gate, w_up, w_down, *shared):
    return layer(tokens, expert_ids, gate_values, w_gate, w_up, w_down[0], *shared)


def layer(
    tokens, expert_ids, gate_values, w_gate, w_up, w_down, shared_gate, shared_up, shared_down
):
    tok_dev, narrow = tokens.shape
    _, _, quarter = w_gate.shape
    experts = lax.axis_size(EXPERT)
    n = lax.axis_size("tensor")
    q = lax.axis_index("tensor").reshape(1)
    w_gate = w_gate.reshape(n, narrow, quarter)
    w_up = w_up.reshape(n, narrow, quarter)

    ids_t = expert_ids.T
    tokens_all = spread(tokens)
    ids_t = expert_ids.T
    arrived = []
    for j, (size, sources) in enumerate(zip(CHUNKS, ([tokens], [tokens, tokens_all[3]]))):
        scratch = [
            pltpu.VMEM(ids_t.shape, jnp.int32),
            pltpu.VMEM(tokens.shape, BF16),
            pltpu.SemaphoreType.DMA((2,)),
        ]
        (rows,) = kernel_call(
            gather_body(experts, sum(CHUNKS[:j]), size),
            [(experts, PAIR, len(sources) * size // PAIR * narrow)],
            ids_t,
            *sources,
            **({} if j else dict(hbm=2, scratch=scratch)),
        )
        arrived.append(exchange(rows, EXPERT))
    columns = kernel_call(columns_body, [(quarter, narrow)] * n, q, w_down, smem=1)
    down = deal(columns)
    weights = kernel_call(
        weight_body(experts),
        [(tok_dev, experts * size) for size in CHUNKS],
        expert_ids,
        gate_values,
    )
    shared_parts = kernel_call(
        shared_body,
        [(tok_dev, narrow)] * n,
        q,
        *tokens_all,
        shared_gate.reshape(n, narrow, -1),
        shared_up.reshape(n, narrow, -1),
        shared_down,
        smem=1,
        flops=10**9,
    )

    returned = []
    for j, (rows, size) in enumerate(zip(arrived, CHUNKS)):
        count = experts * size
        sums_shape = jax.ShapeDtypeStruct((count, 2 * quarter), F32)
        if j == 0:
            left, right, *last = ring(rows)
            args = (rows, left, right)
            bodies = ring_sums_body, ring_hidden_body
        else:
            own_shape = (experts, PAIR, size // PAIR * narrow)
            (own,) = kernel_call(own_body, [own_shape], rows)
            last = shift(own, "tensor", 1), shift(own, "tensor", -1)
            args = (rows,)
            bodies = pair_sums_body, pair_hidden_body
        sums, rest = kernel_call(
            bodies[0],
            [sums_shape, (2 * (1 + j), narrow, quarter)],
            q,
            *args,
            w_gate,
            w_up,
            smem=1,
            flops=10**9,
        )
        (hidden,) = kernel_call(bodies[1], [(count, quarter)], sums, *last, rest, flops=10**9)
        hidden_all = spread(hidden)
        out_shape = (experts, PAIR, size // PAIR * narrow)
        if j == 0:
            (stacked,) = kernel_call(
                stack_copies_body,
                [(n, quarter, narrow)],
                *down,
                hbm=n,
                scratch=[pltpu.SemaphoreType.DMA((n,))],
            )
            scratch = [
                pltpu.VMEM((n, count, quarter), BF16),
                pltpu.VMEM(out_shape, BF16),
                pltpu.SemaphoreType.DMA((n,)),
                pltpu.SemaphoreType.DMA((2,)),
            ]
            (out,) = kernel_call(
                down_body(2),
                [out_shape],
                stacked,
                *hidden_all,
                hbm=n,
                scratch=scratch,
                to_hbm=True,
                flops=10**9,
            )
        else:
            (stacked,) = kernel_call(stack_body, [(n, quarter, narrow)], *down)
            (out,) = kernel_call(near_down_body, [out_shape], *hidden_all, stacked, flops=10**9)
        returned.append(exchange(out, EXPERT))
    shared_all = deal(shared_parts)
    total_shape = jax.ShapeDtypeStruct((tok_dev, narrow), F32)
    (total,) = kernel_call(add_body, [total_shape], weights[0], returned[0], *shared_all)
    return kernel_call(add_body, [(tok_dev, narrow)], weights[1], returned[1], total)[0]


def solution(mesh):
    torus = Mesh(
        mesh.devices.reshape(4, 8, 2, mesh.shape["tensor"]),
        ("expert_0", "expert_1", "expert_2", "tensor"),
    )
    placed = (
        P(EXPERT, "tensor"),
        P(EXPERT, None),
        P(EXPERT, None),
        P(EXPERT, None, "tensor"),
        P(EXPERT, None, "tensor"),
        P(EXPERT, "tensor", None),
        P(None, "tensor"),
        P(None, "tensor"),
        P("tensor", None),
    )
    return jax.shard_map(
        per_device, mesh=torus, in_specs=placed, out_specs=P(EXPERT, "tensor"), check_vma=False
    )
```
